128 devices in a mesh: rows: 16 (over z, y), cols: 8 (over x, core).
Axes of the slice: x: 4, y: 4, z: 4, core: 2. Of those that a mesh axis runs over, the one named last changes fastest.
Arguments:
- grad_stack: float32 [512, 64, 2048], P(None, 'rows', 'cols'), may hold values from -6 to 6
- moment_stack: float32 [512, 64, 2048], P(None, 'rows', 'cols'), may hold values from -6 to 6
- weight_stack: float32 [512, 64, 2048], P(None, 'rows', 'cols'), may hold values from -0.1875 to 0.1875
Outputs:
- new_weights: float32 [512, 64, 2048], P(None, 'rows', 'cols')
- new_momentum: float32 [512, 64, 2048], P(None, 'rows', 'cols')
The draws below stay inside these ranges and needn't reach their ends.
All inputs are finite; a program needn't handle non-finite values.
Results may differ from the reference program's by a relative error of at most 0.0003.
Values sent between devices are 32-bit elements.
A program may use at most 128 MiB of HBM per device.

```python
import jax
import jax.numpy as jnp
from jax import lax

SIDE = 64
WIDE = 2048
MATS = 512
ITERS = 5


def block_levels(rng, extent, shards, least, high):
    loudness, own = 1.0, jax.random.fold_in(rng, 6)
    for axis_at, shards_of in shards:
        steps = jnp.exp(jax.random.uniform(jax.random.fold_in(own, axis_at), (shards_of,), jnp.float32, least / len(shards), high / len(shards)))
        loudness = loudness * jnp.repeat(steps, extent[axis_at] // shards_of).reshape([-1 if axis == axis_at else 1 for axis in range(len(extent))])
    return loudness


def centred(own_key, dims, spread, most, cuts=(), dtype=jnp.bfloat16):
    loudness = block_levels(own_key, dims, cuts, -0.22, 0.18) if cuts else 1.0
    array = jax.random.normal(own_key, dims, jnp.float32) * spread * loudness
    return jnp.minimum(jnp.maximum(array, -most), most).astype(dtype)


def setup_inputs(seed: int = 0) -> dict:
    key_list = jax.random.split(jax.random.key(seed), 4)
    return {
        "grad_stack": centred(key_list[0], (MATS, SIDE, WIDE), 1.0, 6.0, ((1, 16), (2, 8)), jnp.float32),
        "moment_stack": centred(key_list[1], (MATS, SIDE, WIDE), 1.0, 6.0, ((1, 16), (2, 8)), jnp.float32),
        "weight_stack": centred(key_list[2], (MATS, SIDE, WIDE), 0.03, 0.1875, ((1, 16), (2, 8)), jnp.float32),
    }


hold_rate = 0.95
learn_rate = 1.0

def reference(grad_stack, moment_stack, weight_stack):
    new_momentum = hold_rate * moment_stack + grad_stack

    def orthogonal_one(stack):
        iterate = stack[None]
        iterate = iterate * lax.rsqrt(lax.optimization_barrier(jnp.sum(iterate * iterate, axis=(1, 2), keepdims=True)) + 1e-06)
        for step in range(ITERS):
            gram = jnp.einsum('mik,mjk->mij', iterate, iterate, precision=lax.Precision.HIGHEST)
            mixed = -4.775 * gram + 2.0315 * jnp.einsum('mij,mjk->mik', gram, gram, precision=lax.Precision.HIGHEST)
            iterate = 3.4445 * iterate + jnp.einsum('mij,mjk->mik', mixed, iterate, precision=lax.Precision.HIGHEST)
        return iterate[0]
    iterate = lax.map(orthogonal_one, new_momentum)
    new_weights = weight_stack - learn_rate * iterate
    return (new_weights, new_momentum)
```

```python
import functools

import jax
import jax.numpy as jnp
from jax import lax
from jax.experimental import pallas as pl
from jax.experimental.pallas import tpu as pltpu
from jax.sharding import PartitionSpec as P

MESH = pl.DeviceIdType.MESH
HIGHEST = lax.Precision.HIGHEST

hold_rate = 0.95
learn_rate = 1.0
ITERS = 5
CHUNKS = 4
BLOCK = 32


def dot(a, b):
    return jnp.dot(a, b, precision=HIGHEST, preferred_element_type=jnp.float32)


def kernel(nm, back, recv, zbuf, obuf, gsend, gx, fsend, frecv, xsend, xrecv, bsend, brecv, local):
    row, col = lax.axis_index("rows"), lax.axis_index("cols")
    z, y = row // 4, row % 4
    x, core = col // 2, col % 2
    mine = core * 16 + row

    def plane_peer(i):
        to_row = ((z + i // 8) % 4) * 4 + (y + (i // 2) % 4) % 4
        to_core = (core + i % 2) % 2
        return to_row, to_core, {"rows": to_row, "cols": x * 2 + to_core}

    def x_peer(i):
        return {"rows": row, "cols": ((x + i) % 4) * 2 + core}

    def part_of(to_row, to_core, chunk):
        return pl.ds(pl.multiple_of((to_row * 2 + to_core) * (CHUNKS * BLOCK) + chunk * BLOCK, BLOCK), BLOCK)

    barrier = pltpu.get_barrier_semaphore()

    def greet(i, carry):
        pl.semaphore_signal(barrier, inc=1, device_id=plane_peer(i)[2], device_id_type=MESH)
        return carry

    def greet_x(i, carry):
        pl.semaphore_signal(barrier, inc=1, device_id=x_peer(i), device_id_type=MESH)
        return carry

    lax.fori_loop(1, 32, greet, 0)
    lax.fori_loop(1, 4, greet_x, 0)
    pl.semaphore_wait(barrier, 34)

    def send_forward(chunk, carry):
        def one(i, carry):
            to_row, to_core, device = plane_peer(i)
            pltpu.make_async_remote_copy(
                src_ref=nm.at[part_of(to_row, to_core, chunk)],
                dst_ref=recv.at[chunk, mine],
                send_sem=fsend,
                recv_sem=frecv.at[chunk],
                device_id=device,
                device_id_type=MESH,
            ).start()
            return carry

        pltpu.make_async_copy(nm.at[part_of(row, core, chunk)], recv.at[chunk, mine], local.at[chunk]).start()
        return lax.fori_loop(1, 32, one, carry)

    lax.fori_loop(0, CHUNKS, send_forward, 0)

    def roll4(v):
        return pltpu.roll(v, 4, 1)

    low = lax.broadcasted_iota(jnp.int32, (16, 8, 128), 1) < 4
    low8 = lax.broadcasted_iota(jnp.int32, (8, 8, 128), 1) < 4
    at_row = lax.broadcasted_iota(jnp.int32, (128, 128), 0)
    at_col = lax.broadcasted_iota(jnp.int32, (128, 128), 1)
    same = (at_row // 4) % 2 == (at_col // 4) % 2
    eye = jnp.where(at_row == at_col, 1.0, 0.0)
    first = (at_row // 4) % 2 == 0

    def grams(chunk):
        pltpu.make_async_copy(recv.at[chunk, pl.ds(0, 31)], recv.at[chunk, pl.ds(0, 31)], frecv.at[chunk]).wait()
        pltpu.make_async_copy(recv.at[chunk, 0], recv.at[chunk, 0], local.at[chunk]).wait()
        for pair in range(2):
            blocks = []
            for k in range(2):
                a = recv[chunk, 16 * k : 16 * k + 16, 16 * pair : 16 * pair + 8, :]
                b = recv[chunk, 16 * k : 16 * k + 16, 16 * pair + 8 : 16 * pair + 16, :]
                blocks.append(jnp.where(low, a, roll4(b)).reshape(128, 128))
                blocks.append(jnp.where(low, roll4(a), b).reshape(128, 128))
            whole = jnp.concatenate(blocks, axis=1)
            zbuf[chunk, pair] = whole
            gram = lax.dot_general(
                whole, whole, (((1,), (1,)), ((), ())), precision=HIGHEST, preferred_element_type=jnp.float32
            )
            gram = jnp.where(same, gram, 0.0).reshape(8, 2, 8, 128)
            even, odd = gram[:, 0], gram[:, 1]
            even, odd = even + roll4(even), odd + roll4(odd)
            gsend[chunk, 64 * pair : 64 * pair + 64, :] = jnp.where(low8, even, odd).reshape(64, 128)

        def one(i, carry):
            pltpu.make_async_remote_copy(
                src_ref=gsend.at[chunk],
                dst_ref=gx.at[chunk, x],
                send_sem=xsend,
                recv_sem=xrecv.at[chunk],
                device_id=x_peer(i),
                device_id_type=MESH,
            ).start()
            return carry

        lax.fori_loop(1, 4, one, 0)
        gx[chunk, x] = gsend[chunk]

    def finish(chunk):
        pltpu.make_async_copy(gx.at[chunk, pl.ds(0, 3)], gx.at[chunk, pl.ds(0, 3)], xrecv.at[chunk]).wait()
        total = (gx[chunk, 0] + gx[chunk, 1]) + (gx[chunk, 2] + gx[chunk, 3])
        state = []
        for pair in range(2):
            part = total[64 * pair : 64 * pair + 64].reshape(8, 8, 128)
            turned = roll4(part)
            gram = jnp.stack([jnp.where(low8, part, turned), jnp.where(low8, turned, part)], axis=1).reshape(128, 128)
            gram = jnp.where(same, gram, 0.0)
            diag = gram * eye
            one = jnp.sum(jnp.where(first, diag, 0.0), keepdims=True) + 1e-06
            two = jnp.sum(jnp.where(first, 0.0, diag), keepdims=True) + 1e-06
            norm = jnp.where(first, one, two)
            scale = lax.rsqrt(norm)
            state.append([gram * scale * scale, None, scale])
        for step in range(ITERS):
            for one in state:
                gram, total_map, scale = one
                square = dot(gram, gram)
                mixed = 3.4445 * eye - 4.775 * gram + 2.0315 * square
                one[1] = mixed if total_map is None else dot(mixed, total_map)
                if step < ITERS - 1:
                    one[0] = dot(dot(mixed, gram), mixed)
        for pair in range(2):
            out = dot(state[pair][1] * state[pair][2], zbuf[chunk, pair])
            for k in range(2):
                c0 = out[:, 256 * k : 256 * k + 128].reshape(16, 8, 128)
                c1 = out[:, 256 * k + 128 : 256 * k + 256].reshape(16, 8, 128)
                obuf[chunk, 16 * k : 16 * k + 16, 16 * pair : 16 * pair + 8, :] = jnp.where(low, c0, roll4(c1))
                obuf[chunk, 16 * k : 16 * k + 16, 16 * pair + 8 : 16 * pair + 16, :] = jnp.where(low, roll4(c0), c1)

        def one(i, carry):
            to_row, to_core, device = plane_peer(i)
            pltpu.make_async_remote_copy(
                src_ref=obuf.at[chunk, to_core * 16 + to_row],
                dst_ref=back.at[part_of(row, core, chunk)],
                send_sem=bsend,
                recv_sem=brecv,
                device_id=device,
                device_id_type=MESH,
            ).start()
            return carry

        lax.fori_loop(1, 32, one, 0)
        pltpu.make_async_copy(obuf.at[chunk, mine], back.at[part_of(row, core, chunk)], local.at[CHUNKS]).start()

    def step(t, carry):
        @pl.when(t < CHUNKS)
        def _():
            grams(t)

        @pl.when(t > 0)
        def _():
            finish(t - 1)

        return carry

    lax.fori_loop(0, CHUNKS + 1, step, 0)

    def drain(sem, ref):
        pltpu.make_async_copy(ref, ref, sem).wait()

    away = pl.ds(0, 31 * CHUNKS * BLOCK)
    drain(brecv, back.at[away])
    drain(local.at[CHUNKS], back.at[pl.ds(0, CHUNKS * BLOCK)])
    drain(fsend, back.at[away])
    drain(bsend, back.at[away])
    drain(xsend, gx.at[pl.ds(0, 3)])


def exchange(nm):
    f32 = jnp.float32
    return pl.pallas_call(
        kernel,
        out_shape=jax.ShapeDtypeStruct((4096, 128), f32),
        in_specs=[pl.BlockSpec(memory_space=pltpu.VMEM)],
        out_specs=pl.BlockSpec(memory_space=pltpu.VMEM),
        scratch_shapes=[
            pltpu.VMEM((CHUNKS, 32, BLOCK, 128), f32),
            pltpu.VMEM((CHUNKS, 2, 128, 512), f32),
            pltpu.VMEM((CHUNKS, 32, BLOCK, 128), f32),
            pltpu.VMEM((CHUNKS, 128, 128), f32),
            pltpu.VMEM((CHUNKS, 4, 128, 128), f32),
            pltpu.SemaphoreType.DMA,
            pltpu.SemaphoreType.DMA((CHUNKS,)),
            pltpu.SemaphoreType.DMA,
            pltpu.SemaphoreType.DMA((CHUNKS,)),
            pltpu.SemaphoreType.DMA,
            pltpu.SemaphoreType.DMA,
            pltpu.SemaphoreType.DMA((CHUNKS + 1,)),
        ],
        compiler_params=pltpu.CompilerParams(collective_id=0, has_side_effects=True, vmem_limit_bytes=40 * 1024 * 1024),
        name="exchange",
    )(nm)


def flat(a):
    return a.reshape(512, 4, 2, 128).transpose(0, 2, 1, 3).reshape(4096, 128)


def unflat(a):
    return a.reshape(512, 2, 4, 128).transpose(0, 2, 1, 3).reshape(512, 4, 256)


def on_device(grad_stack, moment_stack, weight_stack):
    new_momentum = hold_rate * moment_stack + grad_stack
    back = unflat(exchange(flat(new_momentum)))
    new_weights = weight_stack - learn_rate * back
    return (new_weights, new_momentum)


def solution(mesh):
    placed = (P(None, "rows", "cols"), P(None, "rows", "cols"), P(None, "rows", "cols"))
    return jax.shard_map(
        on_device,
        mesh=mesh,
        in_specs=placed,
        out_specs=(P(None, "rows", "cols"), P(None, "rows", "cols")),
        check_vma=False,
    )
```

```python
import jax
import jax.numpy as jnp
from jax import lax
from jax.experimental import pallas as pl
from jax.experimental.pallas import tpu as pltpu
from jax.sharding import PartitionSpec as P

MESH = pl.DeviceIdType.MESH
HIGHEST = lax.Precision.HIGHEST

hold_rate = 0.95
learn_rate = 1.0
ITERS = 5
CHUNKS = 4


def dot(a, b):
    return jnp.dot(a, b, precision=HIGHEST, preferred_element_type=jnp.float32)


def kernel(
    grad, moment, weight, momentum, result,
    gbuf, mbuf, wbuf, out1, in1, in2, zbuf, out2, in3, in4, gsend, gx,
    load, wload, local, send, recv1, recv2, recv3, recv4, xrecv,
):
    row, col = lax.axis_index("rows"), lax.axis_index("cols")
    z, y = row // 4, row % 4
    x, core = col // 2, col % 2
    first, second = (y, z), (z, y)

    def along_first(half, i):
        to = (first[half] + i) % 4
        to_row = z * 4 + to if half == 0 else to * 4 + y
        return to, {"rows": to_row, "cols": col}

    def along_second(half, i):
        to, to_core = (second[half] + i // 2) % 4, (core + i % 2) % 2
        to_row = to * 4 + y if half == 0 else z * 4 + to
        return to, to_core, {"rows": to_row, "cols": x * 2 + to_core}

    def x_peer(i):
        return {"rows": row, "cols": ((x + i) % 4) * 2 + core}

    def loop(start, stop, body):
        def one(i, carry):
            body(i)
            return carry

        lax.fori_loop(start, stop, one, 0)

    barrier = pltpu.get_barrier_semaphore()

    def greet(device):
        pl.semaphore_signal(barrier, inc=1, device_id=device, device_id_type=MESH)

    for chunk in range(CHUNKS):
        pltpu.make_async_copy(grad.at[:, chunk], gbuf.at[:, chunk], load.at[chunk]).start()
        pltpu.make_async_copy(moment.at[:, chunk], mbuf.at[:, chunk], load.at[CHUNKS + chunk]).start()
    greet({"rows": row, "cols": x * 2 + (core + 1) % 2})
    loop(2, 8, lambda i: greet(along_second(0, i)[2]))
    loop(2, 8, lambda i: greet(along_second(1, i)[2]))
    loop(1, 4, lambda i: greet(x_peer(i)))

    def remote(src, dst, sem, device, which):
        pltpu.make_async_remote_copy(
            src_ref=src, dst_ref=dst, send_sem=send.at[which], recv_sem=sem, device_id=device, device_id_type=MESH
        ).start()

    def drain(ref, sem):
        pltpu.make_async_copy(ref, ref, sem).wait()

    def new_momentum(chunk):
        pltpu.make_async_copy(grad.at[:, chunk], gbuf.at[:, chunk], load.at[chunk]).wait()
        pltpu.make_async_copy(moment.at[:, chunk], mbuf.at[:, chunk], load.at[CHUNKS + chunk]).wait()
        for home in range(32):
            to_z, to_y, to_core = home // 8, (home // 2) % 4, home % 2
            value = hold_rate * mbuf[home, chunk] + gbuf[home, chunk]
            momentum[home, chunk] = value
            out1[chunk, 0, to_y, to_z * 2 + to_core] = value[:16]
            out1[chunk, 1, to_z, to_y * 2 + to_core] = value[16:]

    def send1(chunk):
        for half in range(2):
            own = first[half]
            pltpu.make_async_copy(out1.at[chunk, half, own], in1.at[chunk, half, :, own], local.at[chunk]).start()

        def one(i):
            for half in range(2):
                to, device = along_first(half, i)
                remote(out1.at[chunk, half, to], in1.at[chunk, half, :, first[half]], recv1.at[chunk], device, 0)

        loop(1, 4, one)

    def send2(chunk):
        drain(out1.at[chunk, :, pl.ds(0, 3)], recv1.at[chunk])
        drain(out1.at[chunk, :, 0], local.at[chunk])
        for half in range(2):
            pltpu.make_async_copy(
                in1.at[chunk, half, second[half] * 2 + core],
                in2.at[chunk, half, core * 4 + second[half]],
                local.at[CHUNKS + chunk],
            ).start()

        def one(i):
            for half in range(2):
                to, to_core, device = along_second(half, i)
                remote(
                    in1.at[chunk, half, to * 2 + to_core],
                    in2.at[chunk, half, core * 4 + second[half]],
                    recv2.at[chunk],
                    device,
                    1,
                )

        loop(1, 8, one)

    def send3(chunk):
        for half in range(2):
            pltpu.make_async_copy(
                out2.at[chunk, half, core * 4 + second[half]],
                in3.at[chunk, half, :, second[half] * 2 + core],
                local.at[2 * CHUNKS + chunk],
            ).start()

        def one(i):
            for half in range(2):
                to, to_core, device = along_second(half, i)
                remote(
                    out2.at[chunk, half, to_core * 4 + to],
                    in3.at[chunk, half, :, second[half] * 2 + core],
                    recv3.at[chunk],
                    device,
                    2,
                )

        loop(1, 8, one)

    def send4(chunk):
        drain(out2.at[chunk, :, pl.ds(0, 7)], recv3.at[chunk])
        drain(out2.at[chunk, :, 0], local.at[2 * CHUNKS + chunk])
        for half in range(2):
            own = first[half]
            pltpu.make_async_copy(in3.at[chunk, half, own], in4.at[chunk, half, own], local.at[3 * CHUNKS + chunk]).start()

        def one(i):
            for half in range(2):
                to, device = along_first(half, i)
                remote(in3.at[chunk, half, to], in4.at[chunk, half, first[half]], recv4.at[chunk], device, 3)

        loop(1, 4, one)

    def subtract(chunk):
        drain(in4.at[chunk, :, pl.ds(0, 3)], recv4.at[chunk])
        drain(in4.at[chunk, :, 0], local.at[3 * CHUNKS + chunk])
        for home in range(32):
            to_z, to_y, to_core = home // 8, (home // 2) % 4, home % 2
            result[home, chunk, :16] = wbuf[home, chunk, :16] - learn_rate * in4[chunk, 0, to_y, to_z * 2 + to_core]
            result[home, chunk, 16:] = wbuf[home, chunk, 16:] - learn_rate * in4[chunk, 1, to_z, to_y * 2 + to_core]

    def roll4(v):
        return pltpu.roll(v, 4, 1)

    low = lax.broadcasted_iota(jnp.int32, (16, 8, 128), 1) < 4
    low8 = lax.broadcasted_iota(jnp.int32, (8, 8, 128), 1) < 4
    at_row = lax.broadcasted_iota(jnp.int32, (128, 128), 0)
    at_col = lax.broadcasted_iota(jnp.int32, (128, 128), 1)
    same = (at_row // 4) % 2 == (at_col // 4) % 2
    eye = jnp.where(at_row == at_col, 1.0, 0.0)
    upper = (at_row // 4) % 2 == 0

    def grams(chunk):
        drain(in2.at[chunk, :, pl.ds(0, 7)], recv2.at[chunk])
        drain(in2.at[chunk, :, 0], local.at[CHUNKS + chunk])
        for half in range(2):
            blocks = []
            for k in range(2):
                both = in2[chunk, half, 4 * k : 4 * k + 4].reshape(16, 16, 128)
                a, b = both[:, :8], both[:, 8:]
                blocks.append(jnp.where(low, a, roll4(b)).reshape(128, 128))
                blocks.append(jnp.where(low, roll4(a), b).reshape(128, 128))
            whole = jnp.concatenate(blocks, axis=1)
            zbuf[chunk, half] = whole
            gram = lax.dot_general(
                whole, whole, (((1,), (1,)), ((), ())), precision=HIGHEST, preferred_element_type=jnp.float32
            )
            gram = jnp.where(same, gram, 0.0).reshape(8, 2, 8, 128)
            even, odd = gram[:, 0], gram[:, 1]
            even, odd = even + roll4(even), odd + roll4(odd)
            gsend[chunk, 64 * half : 64 * half + 64, :] = jnp.where(low8, even, odd).reshape(64, 128)
        loop(1, 4, lambda i: remote(gsend.at[chunk], gx.at[chunk, x], xrecv.at[chunk], x_peer(i), 4))
        gx[chunk, x] = gsend[chunk]

    def iterate(chunk):
        drain(gx.at[chunk, pl.ds(0, 3)], xrecv.at[chunk])
        total = (gx[chunk, 0] + gx[chunk, 1]) + (gx[chunk, 2] + gx[chunk, 3])
        state = []
        for half in range(2):
            part = total[64 * half : 64 * half + 64].reshape(8, 8, 128)
            turned = roll4(part)
            gram = jnp.stack([jnp.where(low8, part, turned), jnp.where(low8, turned, part)], axis=1).reshape(128, 128)
            gram = jnp.where(same, gram, 0.0)
            diag = gram * eye
            one = jnp.sum(jnp.where(upper, diag, 0.0), keepdims=True) + 1e-06
            two = jnp.sum(jnp.where(upper, 0.0, diag), keepdims=True) + 1e-06
            scale = lax.rsqrt(jnp.where(upper, one, two))
            state.append([gram * scale * scale, None, scale])
        for step in range(ITERS):
            for one in state:
                gram, product, scale = one
                mixed = 3.4445 * eye - 4.775 * gram + 2.0315 * dot(gram, gram)
                one[1] = mixed if product is None else dot(mixed, product)
                if step < ITERS - 1:
                    one[0] = dot(dot(mixed, gram), mixed)
        return [product * scale for _, product, scale in state]

    def apply(chunk, products):
        for half in range(2):
            out = dot(products[half], zbuf[chunk, half])
            for k in range(2):
                c0 = out[:, 256 * k : 256 * k + 128].reshape(16, 8, 128)
                c1 = out[:, 256 * k + 128 : 256 * k + 256].reshape(16, 8, 128)
                a, b = jnp.where(low, c0, roll4(c1)), jnp.where(low, roll4(c0), c1)
                out2[chunk, half, 4 * k : 4 * k + 4] = jnp.concatenate([a, b], axis=1).reshape(4, 4, 16, 128)

    new_momentum(0)
    pl.semaphore_wait(barrier, 16)
    send1(0)
    new_momentum(1)
    send1(1)
    new_momentum(2)
    new_momentum(3)
    pltpu.make_async_copy(weight, wbuf, wload).start()
    send2(0)
    send1(2)
    send2(1)
    send1(3)
    grams(0)
    send2(2)
    grams(1)

    def step(t):
        products = iterate(t)

        @pl.when(t == 0)
        def _():
            send2(3)

        apply(t, products)
        send3(t)

        @pl.when(t < 2)
        def _():
            grams(t + 2)

        @pl.when(t > 0)
        def _():
            send4(t - 1)

    loop(0, CHUNKS, step)
    send4(3)
    pltpu.make_async_copy(weight, wbuf, wload).wait()
    loop(0, CHUNKS, subtract)

    drain(out1.at[:, :, pl.ds(0, 3)], send.at[0])
    drain(out2.at[:, :, pl.ds(0, 7)], send.at[1])
    drain(out2.at[:, :, pl.ds(0, 7)], send.at[2])
    drain(out1.at[:, :, pl.ds(0, 3)], send.at[3])
    drain(gx.at[:, pl.ds(0, 3)], send.at[4])


def update(grad, moment, weight):
    f32 = jnp.float32
    whole = (32, CHUNKS, 32, 128)
    by_first = (CHUNKS, 2, 4, 8, 16, 128)
    by_second = (CHUNKS, 2, 8, 4, 16, 128)
    dma = pltpu.SemaphoreType.DMA
    return pl.pallas_call(
        kernel,
        out_shape=[jax.ShapeDtypeStruct(whole, f32)] * 2,
        in_specs=[pl.BlockSpec(memory_space=pltpu.HBM)] * 3,
        out_specs=[pl.BlockSpec(memory_space=pltpu.VMEM)] * 2,
        scratch_shapes=[
            pltpu.VMEM(whole, f32),
            pltpu.VMEM(whole, f32),
            pltpu.VMEM(whole, f32),
            pltpu.VMEM(by_first, f32),
            pltpu.VMEM(by_second, f32),
            pltpu.VMEM(by_second, f32),
            pltpu.VMEM((CHUNKS, 2, 128, 512), f32),
            pltpu.VMEM(by_second, f32),
            pltpu.VMEM(by_first, f32),
            pltpu.VMEM(by_first, f32),
            pltpu.VMEM((CHUNKS, 128, 128), f32),
            pltpu.VMEM((CHUNKS, 4, 128, 128), f32),
            dma((2 * CHUNKS,)),
            dma,
            dma((4 * CHUNKS,)),
            dma((5,)),
            dma((CHUNKS,)),
            dma((CHUNKS,)),
            dma((CHUNKS,)),
            dma((CHUNKS,)),
            dma((CHUNKS,)),
        ],
        compiler_params=pltpu.CompilerParams(collective_id=0, has_side_effects=True, vmem_limit_bytes=61000000),
        name="update",
    )(grad, moment, weight)


def tiles(a):
    return a.reshape(512, 4, 2, 128).transpose(0, 2, 1, 3).reshape(32, CHUNKS, 32, 128)


def untiled(a):
    return a.reshape(512, 2, 4, 128).transpose(0, 2, 1, 3).reshape(512, 4, 256)


def on_device(grad_stack, moment_stack, weight_stack):
    momentum, result = update(tiles(grad_stack), tiles(moment_stack), tiles(weight_stack))
    return (untiled(result), untiled(momentum))


def solution(mesh):
    placed = (P(None, "rows", "cols"), P(None, "rows", "cols"), P(None, "rows", "cols"))
    return jax.shard_map(
        on_device,
        mesh=mesh,
        in_specs=placed,
        out_specs=(P(None, "rows", "cols"), P(None, "rows", "cols")),
        check_vma=False,
    )
```

```python
import jax
import jax.numpy as jnp
from jax import lax
from jax.experimental import pallas as pl
from jax.experimental.pallas import tpu as pltpu
from jax.sharding import PartitionSpec as P

MESH = pl.DeviceIdType.MESH
HIGHEST = lax.Precision.HIGHEST

hold_rate = 0.95
learn_rate = 1.0
ITERS = 5
CHUNKS = 4


def split(a):
    high = a.astype(jnp.bfloat16)
    rest = a - high.astype(jnp.float32)
    middle = rest.astype(jnp.bfloat16)
    return high, middle, (rest - middle.astype(jnp.float32)).astype(jnp.bfloat16)


def dot6(a, b):
    (ah, am, al), (bh, bm, bl) = a, b
    n = bh.shape[1]
    wide, small = jnp.concatenate([ah, am], axis=1), jnp.concatenate([ah, al], axis=1)
    top, middle = jnp.concatenate([bh, bh], axis=0), jnp.concatenate([bm, bm], axis=0)
    rest = jnp.dot(small, jnp.concatenate([bl, bh], axis=0), preferred_element_type=jnp.float32)
    if n > 128:
        return (rest + jnp.dot(wide, middle, preferred_element_type=jnp.float32)) + jnp.dot(
            wide, top, preferred_element_type=jnp.float32
        )
    both = jnp.dot(wide, jnp.concatenate([top, middle], axis=1), preferred_element_type=jnp.float32)
    return (rest + both[:, n:]) + both[:, :n]


def kernel(
    grad, moment, weight, momentum, result,
    gbuf, mbuf, wbuf, out1, in1, in2, zbuf, out2, in3, in4, gsend, gx,
    load, wload, local, send, recv1, recv2, recv3, recv4, xrecv,
):
    row, col = lax.axis_index("rows"), lax.axis_index("cols")
    z, y = row // 4, row % 4
    x, core = col // 2, col % 2
    first, second = (y, z), (z, y)

    def along_first(half, i):
        to = (first[half] + i) % 4
        to_row = z * 4 + to if half == 0 else to * 4 + y
        return to, {"rows": to_row, "cols": col}

    def along_second(half, i):
        to, to_core = (second[half] + i // 2) % 4, (core + i % 2) % 2
        to_row = to * 4 + y if half == 0 else z * 4 + to
        return to, to_core, {"rows": to_row, "cols": x * 2 + to_core}

    def x_peer(i):
        return {"rows": row, "cols": ((x + i) % 4) * 2 + core}

    def loop(start, stop, body):
        def one(i, carry):
            body(i)
            return carry

        lax.fori_loop(start, stop, one, 0)

    barrier = pltpu.get_barrier_semaphore()

    def greet(device):
        pl.semaphore_signal(barrier, inc=1, device_id=device, device_id_type=MESH)

    for chunk in range(CHUNKS):
        pltpu.make_async_copy(grad.at[:, chunk], gbuf.at[:, chunk], load.at[chunk]).start()
        pltpu.make_async_copy(moment.at[:, chunk], mbuf.at[:, chunk], load.at[CHUNKS + chunk]).start()
    greet({"rows": row, "cols": x * 2 + (core + 1) % 2})
    loop(2, 8, lambda i: greet(along_second(0, i)[2]))
    loop(2, 8, lambda i: greet(along_second(1, i)[2]))
    loop(1, 4, lambda i: greet(x_peer(i)))

    def remote(src, dst, sem, device, which):
        pltpu.make_async_remote_copy(
            src_ref=src, dst_ref=dst, send_sem=send.at[which], recv_sem=sem, device_id=device, device_id_type=MESH
        ).start()

    def drain(ref, sem):
        pltpu.make_async_copy(ref, ref, sem).wait()

    def new_momentum(chunk):
        pltpu.make_async_copy(grad.at[:, chunk], gbuf.at[:, chunk], load.at[chunk]).wait()
        pltpu.make_async_copy(moment.at[:, chunk], mbuf.at[:, chunk], load.at[CHUNKS + chunk]).wait()
        for home in range(32):
            to_z, to_y, to_core = home // 8, (home // 2) % 4, home % 2
            value = hold_rate * mbuf[home, chunk] + gbuf[home, chunk]
            momentum[home, chunk] = value
            out1[chunk, 0, to_y, to_z * 2 + to_core] = value[:16]
            out1[chunk, 1, to_z, to_y * 2 + to_core] = value[16:]

    def send1(chunk):
        for half in range(2):
            own = first[half]
            pltpu.make_async_copy(out1.at[chunk, half, own], in1.at[chunk, half, :, own], local.at[chunk]).start()

        def one(i):
            for half in range(2):
                to, device = along_first(half, i)
                remote(out1.at[chunk, half, to], in1.at[chunk, half, :, first[half]], recv1.at[chunk], device, 0)

        for i in (2, 1, 3):
            one(i)

    def send2(chunk):
        drain(out1.at[chunk, :, pl.ds(0, 3)], recv1.at[chunk])
        drain(out1.at[chunk, :, 0], local.at[chunk])
        for half in range(2):
            pltpu.make_async_copy(
                in1.at[chunk, half, second[half] * 2 + core],
                in2.at[chunk, half, core * 4 + second[half]],
                local.at[CHUNKS + chunk],
            ).start()

        def one(i):
            for half in range(2):
                to, to_core, device = along_second(half, i)
                remote(
                    in1.at[chunk, half, to * 2 + to_core],
                    in2.at[chunk, half, core * 4 + second[half]],
                    recv2.at[chunk],
                    device,
                    1,
                )

        for i in (4, 5, 2, 3, 6, 7, 1):
            one(i)

    def send3(chunk):
        for half in range(2):
            pltpu.make_async_copy(
                out2.at[chunk, half, core * 4 + second[half]],
                in3.at[chunk, half, :, second[half] * 2 + core],
                local.at[2 * CHUNKS + chunk],
            ).start()

        def one(i):
            for half in range(2):
                to, to_core, device = along_second(half, i)
                remote(
                    out2.at[chunk, half, to_core * 4 + to],
                    in3.at[chunk, half, :, second[half] * 2 + core],
                    recv3.at[chunk],
                    device,
                    2,
                )

        for i in (4, 5, 2, 3, 6, 7, 1):
            one(i)

    def send4(chunk):
        drain(out2.at[chunk, :, pl.ds(0, 7)], recv3.at[chunk])
        drain(out2.at[chunk, :, 0], local.at[2 * CHUNKS + chunk])
        for half in range(2):
            own = first[half]
            pltpu.make_async_copy(in3.at[chunk, half, own], in4.at[chunk, half, own], local.at[3 * CHUNKS + chunk]).start()

        def one(i):
            for half in range(2):
                to, device = along_first(half, i)
                remote(in3.at[chunk, half, to], in4.at[chunk, half, first[half]], recv4.at[chunk], device, 3)

        for i in (2, 1, 3):
            one(i)

    def subtract(chunk):
        drain(in4.at[chunk, :, pl.ds(0, 3)], recv4.at[chunk])
        drain(in4.at[chunk, :, 0], local.at[3 * CHUNKS + chunk])
        for home in range(32):
            to_z, to_y, to_core = home // 8, (home // 2) % 4, home % 2
            result[home, chunk, :16] = wbuf[home, chunk, :16] - learn_rate * in4[chunk, 0, to_y, to_z * 2 + to_core]
            result[home, chunk, 16:] = wbuf[home, chunk, 16:] - learn_rate * in4[chunk, 1, to_z, to_y * 2 + to_core]

    def roll4(v):
        return pltpu.roll(v, 4, 1)

    low = lax.broadcasted_iota(jnp.int32, (16, 8, 128), 1) < 4
    low8 = lax.broadcasted_iota(jnp.int32, (8, 8, 128), 1) < 4
    at_row = lax.broadcasted_iota(jnp.int32, (128, 128), 0)
    at_col = lax.broadcasted_iota(jnp.int32, (128, 128), 1)
    same = (at_row // 4) % 2 == (at_col // 4) % 2
    eye = jnp.where(at_row == at_col, 1.0, 0.0)
    upper = (at_row // 4) % 2 == 0

    def grams(chunk):
        drain(in2.at[chunk, :, pl.ds(0, 7)], recv2.at[chunk])
        drain(in2.at[chunk, :, 0], local.at[CHUNKS + chunk])
        for half in range(2):
            blocks = []
            for k in range(2):
                both = in2[chunk, half, 4 * k : 4 * k + 4].reshape(16, 16, 128)
                a, b = both[:, :8], both[:, 8:]
                blocks.append(jnp.where(low, a, roll4(b)).reshape(128, 128))
                blocks.append(jnp.where(low, roll4(a), b).reshape(128, 128))
            whole = jnp.concatenate(blocks, axis=1)
            zbuf[chunk, half] = whole
            gram = lax.dot_general(
                whole, whole, (((1,), (1,)), ((), ())), precision=HIGHEST, preferred_element_type=jnp.float32
            )
            gram = jnp.where(same, gram, 0.0).reshape(8, 2, 8, 128)
            even, odd = gram[:, 0], gram[:, 1]
            even, odd = even + roll4(even), odd + roll4(odd)
            gsend[chunk, 64 * half : 64 * half + 64, :] = jnp.where(low8, even, odd).reshape(64, 128)
        for i in (2, 1, 3):
            remote(gsend.at[chunk], gx.at[chunk, x], xrecv.at[chunk], x_peer(i), 4)
        gx[chunk, x] = gsend[chunk]

    def iterate(chunk):
        drain(gx.at[chunk, pl.ds(0, 3)], xrecv.at[chunk])
        total = (gx[chunk, 0] + gx[chunk, 1]) + (gx[chunk, 2] + gx[chunk, 3])
        state = []
        for half in range(2):
            part = total[64 * half : 64 * half + 64].reshape(8, 8, 128)
            turned = roll4(part)
            gram = jnp.stack([jnp.where(low8, part, turned), jnp.where(low8, turned, part)], axis=1).reshape(128, 128)
            gram = jnp.where(same, gram, 0.0)
            diag = gram * eye
            one = jnp.sum(jnp.where(upper, diag, 0.0), keepdims=True) + 1e-06
            two = jnp.sum(jnp.where(upper, 0.0, diag), keepdims=True) + 1e-06
            scale = lax.rsqrt(jnp.where(upper, one, two))
            state.append([gram * scale * scale, None, scale])
        grams_now, scales = [one[0] for one in state], [one[2] for one in state]
        products = None
        for step in range(ITERS):
            parts = [split(v) for v in grams_now]
            squares = [dot6(p, p) for p in parts]
            mixed = [3.4445 * eye - 4.775 * g + 2.0315 * s for g, s in zip(grams_now, squares)]
            mixed_parts = [split(v) for v in mixed]
            if step < ITERS - 1:
                turned = [dot6(m, p) for m, p in zip(mixed_parts, parts)]
            if products is None:
                products = mixed
            else:
                products = [dot6(m, split(p)) for m, p in zip(mixed_parts, products)]
            if step < ITERS - 1:
                grams_now = [dot6(split(t), m) for t, m in zip(turned, mixed_parts)]
        return [split(product * scale) for product, scale in zip(products, scales)]

    def apply(chunk, products):
        for half in range(2):
            out = dot6(products[half], split(zbuf[chunk, half]))
            for k in range(2):
                c0 = out[:, 256 * k : 256 * k + 128].reshape(16, 8, 128)
                c1 = out[:, 256 * k + 128 : 256 * k + 256].reshape(16, 8, 128)
                a, b = jnp.where(low, c0, roll4(c1)), jnp.where(low, roll4(c0), c1)
                out2[chunk, half, 4 * k : 4 * k + 4] = jnp.concatenate([a, b], axis=1).reshape(4, 4, 16, 128)

    new_momentum(0)
    pl.semaphore_wait(barrier, 16)
    send1(0)
    new_momentum(1)
    send1(1)
    new_momentum(2)
    new_momentum(3)
    pltpu.make_async_copy(weight, wbuf, wload).start()
    send2(0)
    send2(1)
    send1(2)
    grams(0)
    send1(3)
    grams(1)
    send2(2)

    def step(t):
        products = iterate(t)

        @pl.when(t == 0)
        def _():
            send2(3)

        apply(t, products)
        send3(t)

        @pl.when(t < 2)
        def _():
            grams(t + 2)

        @pl.when(t > 0)
        def _():
            send4(t - 1)

    loop(0, CHUNKS, step)
    send4(3)
    pltpu.make_async_copy(weight, wbuf, wload).wait()
    loop(0, CHUNKS, subtract)

    drain(out1.at[:, :, pl.ds(0, 3)], send.at[0])
    drain(out2.at[:, :, pl.ds(0, 7)], send.at[1])
    drain(out2.at[:, :, pl.ds(0, 7)], send.at[2])
    drain(out1.at[:, :, pl.ds(0, 3)], send.at[3])
    drain(gx.at[:, pl.ds(0, 3)], send.at[4])


def update(grad, moment, weight):
    f32 = jnp.float32
    whole = (32, CHUNKS, 32, 128)
    by_first = (CHUNKS, 2, 4, 8, 16, 128)
    by_second = (CHUNKS, 2, 8, 4, 16, 128)
    dma = pltpu.SemaphoreType.DMA
    return pl.pallas_call(
        kernel,
        out_shape=[jax.ShapeDtypeStruct(whole, f32)] * 2,
        in_specs=[pl.BlockSpec(memory_space=pltpu.HBM)] * 3,
        out_specs=[pl.BlockSpec(memory_space=pltpu.VMEM)] * 2,
        scratch_shapes=[
            pltpu.VMEM(whole, f32),
            pltpu.VMEM(whole, f32),
            pltpu.VMEM(whole, f32),
            pltpu.VMEM(by_first, f32),
            pltpu.VMEM(by_second, f32),
            pltpu.VMEM(by_second, f32),
            pltpu.VMEM((CHUNKS, 2, 128, 512), f32),
            pltpu.VMEM(by_second, f32),
            pltpu.VMEM(by_first, f32),
            pltpu.VMEM(by_first, f32),
            pltpu.VMEM((CHUNKS, 128, 128), f32),
            pltpu.VMEM((CHUNKS, 4, 128, 128), f32),
            dma((2 * CHUNKS,)),
            dma,
            dma((4 * CHUNKS,)),
            dma((5,)),
            dma((CHUNKS,)),
            dma((CHUNKS,)),
            dma((CHUNKS,)),
            dma((CHUNKS,)),
            dma((CHUNKS,)),
        ],
        compiler_params=pltpu.CompilerParams(collective_id=0, has_side_effects=True, vmem_limit_bytes=40 * 1024 * 1024),
        name="update",
    )(grad, moment, weight)


def store(momentum, result, momentum_out, result_out, sems):
    copies = [
        pltpu.make_async_copy(momentum, momentum_out, sems.at[0]),
        pltpu.make_async_copy(result, result_out, sems.at[1]),
    ]
    for copy in copies:
        copy.start()
    for copy in copies:
        copy.wait()


def put_out(momentum, result):
    return pl.pallas_call(
        store,
        out_shape=[jax.ShapeDtypeStruct(momentum.shape, jnp.float32)] * 2,
        in_specs=[pl.BlockSpec(memory_space=pltpu.VMEM)] * 2,
        out_specs=[pl.BlockSpec(memory_space=pl.ANY)] * 2,
        scratch_shapes=[pltpu.SemaphoreType.DMA((2,))],
        compiler_params=pltpu.CompilerParams(vmem_limit_bytes=8 * 1024 * 1024),
        name="put_out",
    )(momentum, result)


def tiles(a):
    return a.reshape(512, 4, 2, 128).transpose(0, 2, 1, 3).reshape(32, CHUNKS, 32, 128)


def untiled(a):
    return a.reshape(512, 2, 4, 128).transpose(0, 2, 1, 3).reshape(512, 4, 256)


def on_device(grad_stack, moment_stack, weight_stack):
    momentum, result = update(*[pltpu.with_memory_space_constraint(tiles(a), pltpu.HBM) for a in (grad_stack, moment_stack, weight_stack)])
    momentum, result = put_out(momentum, result)
    return (untiled(result), untiled(momentum))


def solution(mesh):
    placed = (P(None, "rows", "cols"), P(None, "rows", "cols"), P(None, "rows", "cols"))
    return jax.shard_map(
        on_device,
        mesh=mesh,
        in_specs=placed,
        out_specs=(P(None, "rows", "cols"), P(None, "rows", "cols")),
        check_vma=False,
    )
```

```python
import jax
import jax.numpy as jnp
from jax import lax
from jax.experimental import pallas as pl
from jax.experimental.pallas import tpu as pltpu
from jax.sharding import PartitionSpec as P

MESH = pl.DeviceIdType.MESH
HIGHEST = lax.Precision.HIGHEST

hold_rate = 0.95
learn_rate = 1.0
ITERS = 5
CHUNKS = 4
HUB = 2


def split(a):
    high = a.astype(jnp.bfloat16)
    rest = a - high.astype(jnp.float32)
    middle = rest.astype(jnp.bfloat16)
    return high, middle, (rest - middle.astype(jnp.float32)).astype(jnp.bfloat16)


def dot6(a, b):
    (ah, am, al), (bh, bm, bl) = a, b
    n = bh.shape[1]
    wide, small = jnp.concatenate([ah, am], axis=1), jnp.concatenate([ah, al], axis=1)
    top, middle = jnp.concatenate([bh, bh], axis=0), jnp.concatenate([bm, bm], axis=0)
    rest = jnp.dot(small, jnp.concatenate([bl, bh], axis=0), preferred_element_type=jnp.float32)
    if n > 128:
        return (rest + jnp.dot(wide, middle, preferred_element_type=jnp.float32)) + jnp.dot(
            wide, top, preferred_element_type=jnp.float32
        )
    both = jnp.dot(wide, jnp.concatenate([top, middle], axis=1), preferred_element_type=jnp.float32)
    return (rest + both[:, n:]) + both[:, :n]


def kernel(
    grad, moment, weight, momentum, result,
    gbuf, mbuf, wbuf, out1, in1, in2, zbuf, out2, in3, in4, gsend, gx,
    load, wload, local, send, recv1, recv2, recv3, recv4, xrecv, entered,
):
    row, col = lax.axis_index("rows"), lax.axis_index("cols")
    z, y = row // 4, row % 4
    x, core = col // 2, col % 2
    first, second = (y, z), (z, y)

    def along_first(half, i):
        to = (first[half] + i) % 4
        to_row = z * 4 + to if half == 0 else to * 4 + y
        return to, {"rows": to_row, "cols": col}

    def along_second(half, i):
        to, to_core = (second[half] + i // 2) % 4, (core + i % 2) % 2
        to_row = to * 4 + y if half == 0 else z * 4 + to
        return to, to_core, {"rows": to_row, "cols": x * 2 + to_core}

    def x_peer(i):
        return {"rows": row, "cols": ((x + i) % 4) * 2 + core}

    def loop(start, stop, body):
        def one(i, carry):
            body(i)
            return carry

        lax.fori_loop(start, stop, one, 0)

    barrier = pltpu.get_barrier_semaphore()

    def greet(device):
        pl.semaphore_signal(barrier, inc=1, device_id=device, device_id_type=MESH)

    def fetch(chunk):
        pltpu.make_async_copy(grad.at[:, chunk], gbuf.at[:, chunk], load.at[chunk]).start()
        pltpu.make_async_copy(moment.at[:, chunk], mbuf.at[:, chunk], load.at[CHUNKS + chunk]).start()

    fetch(0)
    for i in (5, 4, 3, 2, 7, 6):
        for half in range(2):
            greet(along_second(half, i)[2])
    greet({"rows": row, "cols": x * 2 + (core + 1) % 2})

    @pl.when(x != HUB)
    def _():
        greet({"rows": row, "cols": HUB * 2 + core})

    for chunk in range(1, CHUNKS):
        fetch(chunk)

    def remote(src, dst, sem, device, which):
        pltpu.make_async_remote_copy(
            src_ref=src, dst_ref=dst, send_sem=send.at[which], recv_sem=sem, device_id=device, device_id_type=MESH
        ).start()

    def drain(ref, sem):
        pltpu.make_async_copy(ref, ref, sem).wait()

    def new_momentum(chunk):
        pltpu.make_async_copy(grad.at[:, chunk], gbuf.at[:, chunk], load.at[chunk]).wait()
        pltpu.make_async_copy(moment.at[:, chunk], mbuf.at[:, chunk], load.at[CHUNKS + chunk]).wait()
        for home in range(32):
            to_z, to_y, to_core = home // 8, (home // 2) % 4, home % 2
            value = hold_rate * mbuf[home, chunk] + gbuf[home, chunk]
            momentum[home, chunk] = value
            out1[chunk, 0, to_y, to_z * 2 + to_core] = value[:16]
            out1[chunk, 1, to_z, to_y * 2 + to_core] = value[16:]

    def send1(chunk):
        for half in range(2):
            own = first[half]
            pltpu.make_async_copy(out1.at[chunk, half, own], in1.at[chunk, half, :, own], local.at[chunk]).start()

        def one(i):
            for half in range(2):
                to, device = along_first(half, i)
                remote(out1.at[chunk, half, to], in1.at[chunk, half, :, first[half]], recv1.at[chunk], device, 0)

        for i in (2, 1, 3):
            one(i)

    def send2(chunk):
        drain(out1.at[chunk, :, pl.ds(0, 3)], recv1.at[chunk])
        drain(out1.at[chunk, :, 0], local.at[chunk])
        for half in range(2):
            pltpu.make_async_copy(
                in1.at[chunk, half, second[half] * 2 + core],
                in2.at[chunk, half, core * 4 + second[half]],
                local.at[CHUNKS + chunk],
            ).start()

        def one(i):
            for half in range(2):
                to, to_core, device = along_second(half, i)
                remote(
                    in1.at[chunk, half, to * 2 + to_core],
                    in2.at[chunk, half, core * 4 + second[half]],
                    recv2.at[chunk],
                    device,
                    1,
                )

        for i in (4, 5, 2, 3, 6, 7, 1):
            one(i)

    def send3(chunk):
        for half in range(2):
            pltpu.make_async_copy(
                out2.at[chunk, half, core * 4 + second[half]],
                in3.at[chunk, half, :, second[half] * 2 + core],
                local.at[2 * CHUNKS + chunk],
            ).start()

        def one(i):
            for half in range(2):
                to, to_core, device = along_second(half, i)
                remote(
                    out2.at[chunk, half, to_core * 4 + to],
                    in3.at[chunk, half, :, second[half] * 2 + core],
                    recv3.at[chunk],
                    device,
                    2,
                )

        for i in (4, 5, 2, 3, 6, 7, 1):
            one(i)

    def send4(chunk):
        drain(out2.at[chunk, :, pl.ds(0, 7)], recv3.at[chunk])
        drain(out2.at[chunk, :, 0], local.at[2 * CHUNKS + chunk])
        for half in range(2):
            own = first[half]
            pltpu.make_async_copy(in3.at[chunk, half, own], in4.at[chunk, half, own], local.at[3 * CHUNKS + chunk]).start()

        def one(i):
            for half in range(2):
                to, device = along_first(half, i)
                remote(in3.at[chunk, half, to], in4.at[chunk, half, first[half]], recv4.at[chunk], device, 3)

        for i in (2, 1, 3):
            one(i)

    def subtract(chunk):
        drain(in4.at[chunk, :, pl.ds(0, 3)], recv4.at[chunk])
        drain(in4.at[chunk, :, 0], local.at[3 * CHUNKS + chunk])
        for home in range(32):
            to_z, to_y, to_core = home // 8, (home // 2) % 4, home % 2
            result[home, chunk, :16] = wbuf[home, chunk, :16] - learn_rate * in4[chunk, 0, to_y, to_z * 2 + to_core]
            result[home, chunk, 16:] = wbuf[home, chunk, 16:] - learn_rate * in4[chunk, 1, to_z, to_y * 2 + to_core]

    def roll4(v):
        return pltpu.roll(v, 4, 1)

    low = lax.broadcasted_iota(jnp.int32, (16, 8, 128), 1) < 4
    low8 = lax.broadcasted_iota(jnp.int32, (8, 8, 128), 1) < 4
    at_row = lax.broadcasted_iota(jnp.int32, (128, 128), 0)
    at_col = lax.broadcasted_iota(jnp.int32, (128, 128), 1)
    same = (at_row // 4) % 2 == (at_col // 4) % 2
    eye = jnp.where(at_row == at_col, 1.0, 0.0)
    upper = (at_row // 4) % 2 == 0

    def grams(chunk):
        drain(in2.at[chunk, :, pl.ds(0, 7)], recv2.at[chunk])
        drain(in2.at[chunk, :, 0], local.at[CHUNKS + chunk])
        for half in range(2):
            blocks = []
            for k in range(2):
                both = in2[chunk, half, 4 * k : 4 * k + 4].reshape(16, 16, 128)
                a, b = both[:, :8], both[:, 8:]
                blocks.append(jnp.where(low, a, roll4(b)).reshape(128, 128))
                blocks.append(jnp.where(low, roll4(a), b).reshape(128, 128))
            whole = jnp.concatenate(blocks, axis=1)
            zbuf[chunk, half] = whole
            gram = lax.dot_general(
                whole, whole, (((1,), (1,)), ((), ())), precision=HIGHEST, preferred_element_type=jnp.float32
            )
            gram = jnp.where(same, gram, 0.0).reshape(8, 2, 8, 128)
            even, odd = gram[:, 0], gram[:, 1]
            even, odd = even + roll4(even), odd + roll4(odd)
            gsend[chunk, 64 * half : 64 * half + 64, :] = jnp.where(low8, even, odd).reshape(64, 128)
        for i in (2, 1, 3):
            remote(gsend.at[chunk], gx.at[chunk, x], xrecv.at[chunk], x_peer(i), 4)
        gx[chunk, x] = gsend[chunk]

    def iterate(chunk):
        drain(gx.at[chunk, pl.ds(0, 3)], xrecv.at[chunk])
        total = (gx[chunk, 0] + gx[chunk, 1]) + (gx[chunk, 2] + gx[chunk, 3])
        state = []
        for half in range(2):
            part = total[64 * half : 64 * half + 64].reshape(8, 8, 128)
            turned = roll4(part)
            gram = jnp.stack([jnp.where(low8, part, turned), jnp.where(low8, turned, part)], axis=1).reshape(128, 128)
            gram = jnp.where(same, gram, 0.0)
            diag = gram * eye
            one = jnp.sum(jnp.where(upper, diag, 0.0), keepdims=True) + 1e-06
            two = jnp.sum(jnp.where(upper, 0.0, diag), keepdims=True) + 1e-06
            scale = lax.rsqrt(jnp.where(upper, one, two))
            state.append([gram * scale * scale, None, scale])
        grams_now, scales = [one[0] for one in state], [one[2] for one in state]
        products = None
        for step in range(ITERS):
            parts = [split(v) for v in grams_now]
            squares = [dot6(p, p) for p in parts]
            mixed = [3.4445 * eye - 4.775 * g + 2.0315 * s for g, s in zip(grams_now, squares)]
            mixed_parts = [split(v) for v in mixed]
            if step < ITERS - 1:
                turned = [dot6(m, p) for m, p in zip(mixed_parts, parts)]
            if products is None:
                products = mixed
            else:
                products = [dot6(m, split(p)) for m, p in zip(mixed_parts, products)]
            if step < ITERS - 1:
                grams_now = [dot6(split(t), m) for t, m in zip(turned, mixed_parts)]
        return [split(product * scale) for product, scale in zip(products, scales)]

    def apply(chunk, products):
        for half in range(2):
            out = dot6(products[half], split(zbuf[chunk, half]))
            for k in range(2):
                c0 = out[:, 256 * k : 256 * k + 128].reshape(16, 8, 128)
                c1 = out[:, 256 * k + 128 : 256 * k + 256].reshape(16, 8, 128)
                a, b = jnp.where(low, c0, roll4(c1)), jnp.where(low, roll4(c0), c1)
                out2[chunk, half, 4 * k : 4 * k + 4] = jnp.concatenate([a, b], axis=1).reshape(4, 4, 16, 128)

    new_momentum(0)

    @pl.when(x != HUB)
    def _():
        pl.semaphore_wait(barrier, 13)

    @pl.when(x == HUB)
    def _():
        pl.semaphore_wait(barrier, 16)
        for i in (2, 1, 3):
            pl.semaphore_signal(entered, inc=1, device_id=x_peer(i), device_id_type=MESH)

    send1(0)
    new_momentum(1)
    send1(1)
    new_momentum(2)
    new_momentum(3)
    pltpu.make_async_copy(weight, wbuf, wload).start()
    send2(0)
    send2(1)
    send1(2)

    @pl.when(x != HUB)
    def _():
        pl.semaphore_wait(entered, 1)

    grams(0)
    send1(3)
    grams(1)
    send2(2)

    def step(t):
        products = iterate(t)

        @pl.when(t == 0)
        def _():
            send2(3)

        apply(t, products)
        send3(t)

        @pl.when(t < 2)
        def _():
            grams(t + 2)

        @pl.when(t > 0)
        def _():
            send4(t - 1)

    loop(0, CHUNKS, step)
    send4(3)
    pltpu.make_async_copy(weight, wbuf, wload).wait()
    loop(0, CHUNKS, subtract)

    drain(out1.at[:, :, pl.ds(0, 3)], send.at[0])
    drain(out2.at[:, :, pl.ds(0, 7)], send.at[1])
    drain(out2.at[:, :, pl.ds(0, 7)], send.at[2])
    drain(out1.at[:, :, pl.ds(0, 3)], send.at[3])
    drain(gx.at[:, pl.ds(0, 3)], send.at[4])


def update(grad, moment, weight):
    f32 = jnp.float32
    whole = (32, CHUNKS, 32, 128)
    by_first = (CHUNKS, 2, 4, 8, 16, 128)
    by_second = (CHUNKS, 2, 8, 4, 16, 128)
    dma = pltpu.SemaphoreType.DMA
    return pl.pallas_call(
        kernel,
        out_shape=[jax.ShapeDtypeStruct(whole, f32)] * 2,
        in_specs=[pl.BlockSpec(memory_space=pltpu.HBM)] * 3,
        out_specs=[pl.BlockSpec(memory_space=pltpu.VMEM)] * 2,
        scratch_shapes=[
            pltpu.VMEM(whole, f32),
            pltpu.VMEM(whole, f32),
            pltpu.VMEM(whole, f32),
            pltpu.VMEM(by_first, f32),
            pltpu.VMEM(by_second, f32),
            pltpu.VMEM(by_second, f32),
            pltpu.VMEM((CHUNKS, 2, 128, 512), f32),
            pltpu.VMEM(by_second, f32),
            pltpu.VMEM(by_first, f32),
            pltpu.VMEM(by_first, f32),
            pltpu.VMEM((CHUNKS, 128, 128), f32),
            pltpu.VMEM((CHUNKS, 4, 128, 128), f32),
            dma((2 * CHUNKS,)),
            dma,
            dma((4 * CHUNKS,)),
            dma((5,)),
            dma((CHUNKS,)),
            dma((CHUNKS,)),
            dma((CHUNKS,)),
            dma((CHUNKS,)),
            dma((CHUNKS,)),
            pltpu.SemaphoreType.REGULAR,
        ],
        compiler_params=pltpu.CompilerParams(collective_id=0, has_side_effects=True, vmem_limit_bytes=40 * 1024 * 1024),
        name="update",
    )(grad, moment, weight)


def store(momentum, result, momentum_out, result_out, sems):
    copies = []
    for part in range(4):
        at = pl.ds(8 * part, 8)
        copies.append(pltpu.make_async_copy(momentum.at[at], momentum_out.at[at], sems.at[part]))
        copies.append(pltpu.make_async_copy(result.at[at], result_out.at[at], sems.at[4 + part]))
    for copy in copies:
        copy.start()
    for copy in copies:
        copy.wait()


def put_out(momentum, result):
    return pl.pallas_call(
        store,
        out_shape=[jax.ShapeDtypeStruct(momentum.shape, jnp.float32)] * 2,
        in_specs=[pl.BlockSpec(memory_space=pltpu.VMEM)] * 2,
        out_specs=[pl.BlockSpec(memory_space=pl.ANY)] * 2,
        scratch_shapes=[pltpu.SemaphoreType.DMA((8,))],
        compiler_params=pltpu.CompilerParams(vmem_limit_bytes=8 * 1024 * 1024),
        name="put_out",
    )(momentum, result)


def tiles(a):
    return a.reshape(512, 4, 2, 128).transpose(0, 2, 1, 3).reshape(32, CHUNKS, 32, 128)


def untiled(a):
    return a.reshape(512, 2, 4, 128).transpose(0, 2, 1, 3).reshape(512, 4, 256)


def on_device(grad_stack, moment_stack, weight_stack):
    momentum, result = update(*[pltpu.with_memory_space_constraint(tiles(a), pltpu.HBM) for a in (grad_stack, moment_stack, weight_stack)])
    momentum, result = put_out(momentum, result)
    return (untiled(result), untiled(momentum))


def solution(mesh):
    placed = (P(None, "rows", "cols"), P(None, "rows", "cols"), P(None, "rows", "cols"))
    return jax.shard_map(
        on_device,
        mesh=mesh,
        in_specs=placed,
        out_specs=(P(None, "rows", "cols"), P(None, "rows", "cols")),
        check_vma=False,
    )
```

```python
import jax
import jax.numpy as jnp
from jax import lax
from jax.experimental import pallas as pl
from jax.experimental.pallas import tpu as pltpu
from jax.sharding import PartitionSpec as P

MESH = pl.DeviceIdType.MESH
HIGHEST = lax.Precision.HIGHEST

hold_rate = 0.95
learn_rate = 1.0
ITERS = 5
CHUNKS = 4
HUB = 2


def split(a):
    high = a.astype(jnp.bfloat16)
    rest = a - high.astype(jnp.float32)
    middle = rest.astype(jnp.bfloat16)
    return high, middle, (rest - middle.astype(jnp.float32)).astype(jnp.bfloat16)


def dot6(a, b):
    (ah, am, al), (bh, bm, bl) = a, b
    n = bh.shape[1]
    wide, small = jnp.concatenate([ah, am], axis=1), jnp.concatenate([ah, al], axis=1)
    top, middle = jnp.concatenate([bh, bh], axis=0), jnp.concatenate([bm, bm], axis=0)
    rest = jnp.dot(small, jnp.concatenate([bl, bh], axis=0), preferred_element_type=jnp.float32)
    if n > 128:
        return (rest + jnp.dot(wide, middle, preferred_element_type=jnp.float32)) + jnp.dot(
            wide, top, preferred_element_type=jnp.float32
        )
    both = jnp.dot(wide, jnp.concatenate([top, middle], axis=1), preferred_element_type=jnp.float32)
    return (rest + both[:, n:]) + both[:, :n]


def kernel(
    grad, moment, weight, momentum, result,
    gbuf, mbuf, wbuf, out1, in1, in2, zbuf, out2, in3, in4, gsend, gx,
    load, wload, local, send, recv1, recv2, recv3, recv4, xrecv, entered,
):
    row, col = lax.axis_index("rows"), lax.axis_index("cols")
    z, y = row // 4, row % 4
    x, core = col // 2, col % 2
    first, second = (y, z), (z, y)

    def along_first(half, i):
        to = (first[half] + i) % 4
        to_row = z * 4 + to if half == 0 else to * 4 + y
        return to, {"rows": to_row, "cols": col}

    def along_second(half, i):
        to, to_core = (second[half] + i // 2) % 4, (core + i % 2) % 2
        to_row = to * 4 + y if half == 0 else z * 4 + to
        return to, to_core, {"rows": to_row, "cols": x * 2 + to_core}

    def x_peer(i):
        return {"rows": row, "cols": ((x + i) % 4) * 2 + core}

    def loop(start, stop, body):
        def one(i, carry):
            body(i)
            return carry

        lax.fori_loop(start, stop, one, 0)

    barrier = pltpu.get_barrier_semaphore()

    def greet(device):
        pl.semaphore_signal(barrier, inc=1, device_id=device, device_id_type=MESH)

    def fetch(chunk):
        pltpu.make_async_copy(grad.at[:, chunk], gbuf.at[:, chunk], load.at[chunk]).start()
        pltpu.make_async_copy(moment.at[:, chunk], mbuf.at[:, chunk], load.at[CHUNKS + chunk]).start()

    fetch(0)
    for i in (5, 4, 3, 2, 7, 6):
        for half in range(2):
            greet(along_second(half, i)[2])
    greet({"rows": row, "cols": x * 2 + (core + 1) % 2})

    @pl.when(x != HUB)
    def _():
        greet({"rows": row, "cols": HUB * 2 + core})

    for chunk in range(1, CHUNKS):
        fetch(chunk)

    def remote(src, dst, sem, device, which):
        pltpu.make_async_remote_copy(
            src_ref=src, dst_ref=dst, send_sem=send.at[which], recv_sem=sem, device_id=device, device_id_type=MESH
        ).start()

    def drain(ref, sem):
        pltpu.make_async_copy(ref, ref, sem).wait()

    def new_momentum(chunk):
        pltpu.make_async_copy(grad.at[:, chunk], gbuf.at[:, chunk], load.at[chunk]).wait()
        pltpu.make_async_copy(moment.at[:, chunk], mbuf.at[:, chunk], load.at[CHUNKS + chunk]).wait()
        for home in range(32):
            to_z, to_y, to_core = home // 8, (home // 2) % 4, home % 2
            value = hold_rate * mbuf[home, chunk] + gbuf[home, chunk]
            momentum[home, chunk] = value
            out1[chunk, 0, to_y, to_z * 2 + to_core] = value[:16]
            out1[chunk, 1, to_z, to_y * 2 + to_core] = value[16:]

    def send1(chunk):
        for half in range(2):
            own = first[half]
            pltpu.make_async_copy(out1.at[chunk, half, own], in1.at[chunk, half, :, own], local.at[chunk]).start()

        def one(i):
            for half in range(2):
                to, device = along_first(half, i)
                remote(out1.at[chunk, half, to], in1.at[chunk, half, :, first[half]], recv1.at[chunk], device, 0)

        for i in (2, 1, 3):
            one(i)

    def send2(chunk):
        drain(out1.at[chunk, :, pl.ds(0, 3)], recv1.at[chunk])
        drain(out1.at[chunk, :, 0], local.at[chunk])
        for half in range(2):
            pltpu.make_async_copy(
                in1.at[chunk, half, second[half] * 2 + core],
                in2.at[chunk, half, core * 4 + second[half]],
                local.at[CHUNKS + chunk],
            ).start()

        def one(i):
            for half in range(2):
                to, to_core, device = along_second(half, i)
                remote(
                    in1.at[chunk, half, to * 2 + to_core],
                    in2.at[chunk, half, core * 4 + second[half]],
                    recv2.at[chunk],
                    device,
                    1,
                )

        for i in (4, 5, 2, 3, 6, 7, 1):
            one(i)

    def send3(chunk):
        for half in range(2):
            pltpu.make_async_copy(
                out2.at[chunk, half, core * 4 + second[half]],
                in3.at[chunk, half, :, second[half] * 2 + core],
                local.at[2 * CHUNKS + chunk],
            ).start()

        def one(i):
            for half in range(2):
                to, to_core, device = along_second(half, i)
                remote(
                    out2.at[chunk, half, to_core * 4 + to],
                    in3.at[chunk, half, :, second[half] * 2 + core],
                    recv3.at[chunk],
                    device,
                    2,
                )

        for i in (4, 5, 2, 3, 6, 7, 1):
            one(i)

    def send4(chunk):
        drain(out2.at[chunk, :, pl.ds(0, 7)], recv3.at[chunk])
        drain(out2.at[chunk, :, 0], local.at[2 * CHUNKS + chunk])
        for half in range(2):
            own = first[half]
            pltpu.make_async_copy(in3.at[chunk, half, own], in4.at[chunk, half, own], local.at[3 * CHUNKS + chunk]).start()

        def one(i):
            for half in range(2):
                to, device = along_first(half, i)
                remote(in3.at[chunk, half, to], in4.at[chunk, half, first[half]], recv4.at[chunk], device, 3)

        for i in (2, 1, 3):
            one(i)

    def subtract(chunk):
        drain(in4.at[chunk, :, pl.ds(0, 3)], recv4.at[chunk])
        drain(in4.at[chunk, :, 0], local.at[3 * CHUNKS + chunk])
        for home in range(32):
            to_z, to_y, to_core = home // 8, (home // 2) % 4, home % 2
            result[home, chunk, :16] = wbuf[home, chunk, :16] - learn_rate * in4[chunk, 0, to_y, to_z * 2 + to_core]
            result[home, chunk, 16:] = wbuf[home, chunk, 16:] - learn_rate * in4[chunk, 1, to_z, to_y * 2 + to_core]

    def roll4(v):
        return pltpu.roll(v, 4, 1)

    low = lax.broadcasted_iota(jnp.int32, (16, 8, 128), 1) < 4
    low8 = lax.broadcasted_iota(jnp.int32, (8, 8, 128), 1) < 4
    at_row = lax.broadcasted_iota(jnp.int32, (128, 128), 0)
    at_col = lax.broadcasted_iota(jnp.int32, (128, 128), 1)
    same = (at_row // 4) % 2 == (at_col // 4) % 2
    eye = jnp.where(at_row == at_col, 1.0, 0.0)
    upper = (at_row // 4) % 2 == 0

    def grams(chunk):
        drain(in2.at[chunk, :, pl.ds(0, 7)], recv2.at[chunk])
        drain(in2.at[chunk, :, 0], local.at[CHUNKS + chunk])
        for half in range(2):
            blocks = []
            for k in range(2):
                both = in2[chunk, half, 4 * k : 4 * k + 4].reshape(16, 16, 128)
                a, b = both[:, :8], both[:, 8:]
                blocks.append(jnp.where(low, a, roll4(b)).reshape(128, 128))
                blocks.append(jnp.where(low, roll4(a), b).reshape(128, 128))
            whole = jnp.concatenate(blocks, axis=1)
            zbuf[chunk, half] = whole
            gram = lax.dot_general(
                whole, whole, (((1,), (1,)), ((), ())), precision=HIGHEST, preferred_element_type=jnp.float32
            )
            gram = jnp.where(same, gram, 0.0).reshape(8, 2, 8, 128)
            even, odd = gram[:, 0], gram[:, 1]
            even, odd = even + roll4(even), odd + roll4(odd)
            gsend[chunk, 64 * half : 64 * half + 64, :] = jnp.where(low8, even, odd).reshape(64, 128)
        gx[chunk, x] = gsend[chunk]
        for i in (2, 1, 3):
            remote(gsend.at[chunk], gx.at[chunk, x], xrecv.at[chunk], x_peer(i), 4)

    def iterate(chunk):
        drain(gx.at[chunk, pl.ds(0, 3)], xrecv.at[chunk])
        total = (gx[chunk, 0] + gx[chunk, 1]) + (gx[chunk, 2] + gx[chunk, 3])
        state = []
        for half in range(2):
            part = total[64 * half : 64 * half + 64].reshape(8, 8, 128)
            turned = roll4(part)
            gram = jnp.stack([jnp.where(low8, part, turned), jnp.where(low8, turned, part)], axis=1).reshape(128, 128)
            gram = jnp.where(same, gram, 0.0)
            diag = gram * eye
            one = jnp.sum(jnp.where(upper, diag, 0.0), keepdims=True) + 1e-06
            two = jnp.sum(jnp.where(upper, 0.0, diag), keepdims=True) + 1e-06
            scale = lax.rsqrt(jnp.where(upper, one, two))
            state.append([gram * scale * scale, None, scale])
        grams_now, scales = [one[0] for one in state], [one[2] for one in state]
        products = None
        for step in range(ITERS):
            parts = [split(v) for v in grams_now]
            squares = [dot6(p, p) for p in parts]
            mixed = [3.4445 * eye - 4.775 * g + 2.0315 * s for g, s in zip(grams_now, squares)]
            mixed_parts = [split(v) for v in mixed]
            if step < ITERS - 1:
                turned = [dot6(m, p) for m, p in zip(mixed_parts, parts)]
            if products is None:
                products = mixed
            else:
                products = [dot6(m, split(p)) for m, p in zip(mixed_parts, products)]
            if step < ITERS - 1:
                grams_now = [dot6(split(t), m) for t, m in zip(turned, mixed_parts)]
        return [split(product * scale) for product, scale in zip(products, scales)]

    def apply(chunk, products):
        for half in range(2):
            out = dot6(products[half], split(zbuf[chunk, half]))
            for k in range(2):
                c0 = out[:, 256 * k : 256 * k + 128].reshape(16, 8, 128)
                c1 = out[:, 256 * k + 128 : 256 * k + 256].reshape(16, 8, 128)
                a, b = jnp.where(low, c0, roll4(c1)), jnp.where(low, roll4(c0), c1)
                out2[chunk, half, 4 * k : 4 * k + 4] = jnp.concatenate([a, b], axis=1).reshape(4, 4, 16, 128)

    new_momentum(0)

    @pl.when(x != HUB)
    def _():
        pl.semaphore_wait(barrier, 13)

    @pl.when(x == HUB)
    def _():
        pl.semaphore_wait(barrier, 16)
        for i in (2, 1, 3):
            pl.semaphore_signal(entered, inc=1, device_id=x_peer(i), device_id_type=MESH)

    send1(0)
    new_momentum(1)
    send1(1)
    new_momentum(2)
    new_momentum(3)
    pltpu.make_async_copy(weight, wbuf, wload).start()
    send2(0)
    send2(1)
    send1(2)
    send1(3)

    @pl.when(x != HUB)
    def _():
        pl.semaphore_wait(entered, 1)

    grams(0)
    grams(1)
    send2(2)

    def step(t):
        products = iterate(t)

        @pl.when(t == 0)
        def _():
            send2(3)

        apply(t, products)
        send3(t)

        @pl.when(t < 2)
        def _():
            grams(t + 2)

        @pl.when((t > 0) & (t < 3))
        def _():
            send4(t - 1)

    loop(0, CHUNKS, step)
    send4(2)
    send4(3)
    pltpu.make_async_copy(weight, wbuf, wload).wait()
    loop(0, CHUNKS, subtract)

    drain(out1.at[:, :, pl.ds(0, 3)], send.at[0])
    drain(out2.at[:, :, pl.ds(0, 7)], send.at[1])
    drain(out2.at[:, :, pl.ds(0, 7)], send.at[2])
    drain(out1.at[:, :, pl.ds(0, 3)], send.at[3])
    drain(gx.at[:, pl.ds(0, 3)], send.at[4])


def update(grad, moment, weight):
    f32 = jnp.float32
    whole = (32, CHUNKS, 32, 128)
    by_first = (CHUNKS, 2, 4, 8, 16, 128)
    by_second = (CHUNKS, 2, 8, 4, 16, 128)
    dma = pltpu.SemaphoreType.DMA
    return pl.pallas_call(
        kernel,
        out_shape=[jax.ShapeDtypeStruct(whole, f32)] * 2,
        in_specs=[pl.BlockSpec(memory_space=pltpu.HBM)] * 3,
        out_specs=[pl.BlockSpec(memory_space=pltpu.VMEM)] * 2,
        scratch_shapes=[
            pltpu.VMEM(whole, f32),
            pltpu.VMEM(whole, f32),
            pltpu.VMEM(whole, f32),
            pltpu.VMEM(by_first, f32),
            pltpu.VMEM(by_second, f32),
            pltpu.VMEM(by_second, f32),
            pltpu.VMEM((CHUNKS, 2, 128, 512), f32),
            pltpu.VMEM(by_second, f32),
            pltpu.VMEM(by_first, f32),
            pltpu.VMEM(by_first, f32),
            pltpu.VMEM((CHUNKS, 128, 128), f32),
            pltpu.VMEM((CHUNKS, 4, 128, 128), f32),
            dma((2 * CHUNKS,)),
            dma,
            dma((4 * CHUNKS,)),
            dma((5,)),
            dma((CHUNKS,)),
            dma((CHUNKS,)),
            dma((CHUNKS,)),
            dma((CHUNKS,)),
            dma((CHUNKS,)),
            pltpu.SemaphoreType.REGULAR,
        ],
        compiler_params=pltpu.CompilerParams(collective_id=0, has_side_effects=True, vmem_limit_bytes=40 * 1024 * 1024),
        name="update",
    )(grad, moment, weight)


def store(momentum, result, momentum_out, result_out, sems):
    copies = []
    for part in range(4):
        at = pl.ds(8 * part, 8)
        copies.append(pltpu.make_async_copy(momentum.at[at], momentum_out.at[at], sems.at[part]))
        copies.append(pltpu.make_async_copy(result.at[at], result_out.at[at], sems.at[4 + part]))
    for copy in copies:
        copy.start()
    for copy in copies:
        copy.wait()


def put_out(momentum, result):
    return pl.pallas_call(
        store,
        out_shape=[jax.ShapeDtypeStruct(momentum.shape, jnp.float32)] * 2,
        in_specs=[pl.BlockSpec(memory_space=pltpu.VMEM)] * 2,
        out_specs=[pl.BlockSpec(memory_space=pl.ANY)] * 2,
        scratch_shapes=[pltpu.SemaphoreType.DMA((8,))],
        compiler_params=pltpu.CompilerParams(vmem_limit_bytes=8 * 1024 * 1024),
        name="put_out",
    )(momentum, result)


def tiles(a):
    return a.reshape(512, 4, 2, 128).transpose(0, 2, 1, 3).reshape(32, CHUNKS, 32, 128)


def untiled(a):
    return a.reshape(512, 2, 4, 128).transpose(0, 2, 1, 3).reshape(512, 4, 256)


def on_device(grad_stack, moment_stack, weight_stack):
    momentum, result = update(*[pltpu.with_memory_space_constraint(tiles(a), pltpu.HBM) for a in (grad_stack, moment_stack, weight_stack)])
    momentum, result = put_out(momentum, result)
    return (untiled(result), untiled(momentum))


def solution(mesh):
    placed = (P(None, "rows", "cols"), P(None, "rows", "cols"), P(None, "rows", "cols"))
    return jax.shard_map(
        on_device,
        mesh=mesh,
        in_specs=placed,
        out_specs=(P(None, "rows", "cols"), P(None, "rows", "cols")),
        check_vma=False,
    )
```

```python
import jax
import jax.numpy as jnp
from jax import lax
from jax.experimental import pallas as pl
from jax.experimental.pallas import tpu as pltpu
from jax.sharding import PartitionSpec as P

MESH = pl.DeviceIdType.MESH
HIGHEST = lax.Precision.HIGHEST

hold_rate = 0.95
learn_rate = 1.0
ITERS = 5
CHUNKS = 4
HUB = 2


def split(a):
    high = a.astype(jnp.bfloat16)
    rest = a - high.astype(jnp.float32)
    middle = rest.astype(jnp.bfloat16)
    return high, middle, (rest - middle.astype(jnp.float32)).astype(jnp.bfloat16)


def dot6(a, b):
    (ah, am, al), (bh, bm, bl) = a, b
    n = bh.shape[1]
    wide, small = jnp.concatenate([ah, am], axis=1), jnp.concatenate([ah, al], axis=1)
    top, middle = jnp.concatenate([bh, bh], axis=0), jnp.concatenate([bm, bm], axis=0)
    rest = jnp.dot(small, jnp.concatenate([bl, bh], axis=0), preferred_element_type=jnp.float32)
    if n > 128:
        return (rest + jnp.dot(wide, middle, preferred_element_type=jnp.float32)) + jnp.dot(
            wide, top, preferred_element_type=jnp.float32
        )
    both = jnp.dot(wide, jnp.concatenate([top, middle], axis=1), preferred_element_type=jnp.float32)
    return (rest + both[:, n:]) + both[:, :n]


def kernel(
    grad, moment, weight, momentum, result,
    gbuf, mbuf, wbuf, out1, in1, in2, zbuf, out2, in3, in4, gsend, gx,
    load, wload, local, send, recv1, recv2, recv3, recv4, xrecv, entered,
):
    row, col = lax.axis_index("rows"), lax.axis_index("cols")
    z, y = row // 4, row % 4
    x, core = col // 2, col % 2
    first, second = (y, z), (z, y)

    def along_first(half, i):
        to = (first[half] + i) % 4
        to_row = z * 4 + to if half == 0 else to * 4 + y
        return to, {"rows": to_row, "cols": col}

    def along_second(half, i):
        to, to_core = (second[half] + i // 2) % 4, (core + i % 2) % 2
        to_row = to * 4 + y if half == 0 else z * 4 + to
        return to, to_core, {"rows": to_row, "cols": x * 2 + to_core}

    def x_peer(i):
        return {"rows": row, "cols": ((x + i) % 4) * 2 + core}

    def loop(start, stop, body):
        def one(i, carry):
            body(i)
            return carry

        lax.fori_loop(start, stop, one, 0)

    barrier = pltpu.get_barrier_semaphore()

    def greet(device):
        pl.semaphore_signal(barrier, inc=1, device_id=device, device_id_type=MESH)

    def fetch(chunk):
        pltpu.make_async_copy(grad.at[:, chunk], gbuf.at[:, chunk], load.at[chunk]).start()
        pltpu.make_async_copy(moment.at[:, chunk], mbuf.at[:, chunk], load.at[CHUNKS + chunk]).start()

    fetch(0)
    for i in (5, 4, 3, 2, 7, 6):
        for half in range(2):
            greet(along_second(half, i)[2])
    greet({"rows": row, "cols": x * 2 + (core + 1) % 2})

    @pl.when(x != HUB)
    def _():
        greet({"rows": row, "cols": HUB * 2 + core})

    for chunk in range(1, CHUNKS):
        fetch(chunk)

    def remote(src, dst, sem, device, which):
        pltpu.make_async_remote_copy(
            src_ref=src, dst_ref=dst, send_sem=send.at[which], recv_sem=sem, device_id=device, device_id_type=MESH
        ).start()

    def drain(ref, sem):
        pltpu.make_async_copy(ref, ref, sem).wait()

    def new_momentum(chunk):
        pltpu.make_async_copy(grad.at[:, chunk], gbuf.at[:, chunk], load.at[chunk]).wait()
        pltpu.make_async_copy(moment.at[:, chunk], mbuf.at[:, chunk], load.at[CHUNKS + chunk]).wait()
        for home in range(32):
            to_z, to_y, to_core = home // 8, (home // 2) % 4, home % 2
            value = hold_rate * mbuf[home, chunk] + gbuf[home, chunk]
            momentum[home, chunk] = value
            out1[chunk, 0, to_y, to_z * 2 + to_core] = value[:16]
            out1[chunk, 1, to_z, to_y * 2 + to_core] = value[16:]

    def send1(chunk):
        for half in range(2):
            own = first[half]
            pltpu.make_async_copy(out1.at[chunk, half, own], in1.at[chunk, half, :, own], local.at[chunk]).start()

        def one(i):
            for half in range(2):
                to, device = along_first(half, i)
                remote(out1.at[chunk, half, to], in1.at[chunk, half, :, first[half]], recv1.at[chunk], device, 0)

        for i in (2, 1, 3):
            one(i)

    def send2(chunk):
        drain(out1.at[chunk, :, pl.ds(0, 3)], recv1.at[chunk])
        drain(out1.at[chunk, :, 0], local.at[chunk])
        for half in range(2):
            pltpu.make_async_copy(
                in1.at[chunk, half, second[half] * 2 + core],
                in2.at[chunk, half, core * 4 + second[half]],
                local.at[CHUNKS + chunk],
            ).start()

        def one(i):
            for half in range(2):
                to, to_core, device = along_second(half, i)
                remote(
                    in1.at[chunk, half, to * 2 + to_core],
                    in2.at[chunk, half, core * 4 + second[half]],
                    recv2.at[chunk],
                    device,
                    1,
                )

        for i in (4, 5, 2, 3, 6, 7, 1):
            one(i)

    def send3(chunk):
        for half in range(2):
            pltpu.make_async_copy(
                out2.at[chunk, half, core * 4 + second[half]],
                in3.at[chunk, half, :, second[half] * 2 + core],
                local.at[2 * CHUNKS + chunk],
            ).start()

        def one(i):
            for half in range(2):
                to, to_core, device = along_second(half, i)
                remote(
                    out2.at[chunk, half, to_core * 4 + to],
                    in3.at[chunk, half, :, second[half] * 2 + core],
                    recv3.at[chunk],
                    device,
                    2,
                )

        for i in (4, 5, 2, 3, 6, 7, 1):
            one(i)

    def send4(chunk):
        drain(out2.at[chunk, :, pl.ds(0, 7)], recv3.at[chunk])
        drain(out2.at[chunk, :, 0], local.at[2 * CHUNKS + chunk])
        for half in range(2):
            own = first[half]
            pltpu.make_async_copy(in3.at[chunk, half, own], in4.at[chunk, half, own], local.at[3 * CHUNKS + chunk]).start()

        def one(i):
            for half in range(2):
                to, device = along_first(half, i)
                remote(in3.at[chunk, half, to], in4.at[chunk, half, first[half]], recv4.at[chunk], device, 3)

        for i in (2, 1, 3):
            one(i)

    def subtract(chunk):
        drain(in4.at[chunk, :, pl.ds(0, 3)], recv4.at[chunk])
        drain(in4.at[chunk, :, 0], local.at[3 * CHUNKS + chunk])
        for home in range(32):
            to_z, to_y, to_core = home // 8, (home // 2) % 4, home % 2
            result[home, chunk, :16] = wbuf[home, chunk, :16] - learn_rate * in4[chunk, 0, to_y, to_z * 2 + to_core]
            result[home, chunk, 16:] = wbuf[home, chunk, 16:] - learn_rate * in4[chunk, 1, to_z, to_y * 2 + to_core]

    def roll4(v):
        return pltpu.roll(v, 4, 1)

    low = lax.broadcasted_iota(jnp.int32, (16, 8, 128), 1) < 4
    low8 = lax.broadcasted_iota(jnp.int32, (8, 8, 128), 1) < 4
    at_row = lax.broadcasted_iota(jnp.int32, (128, 128), 0)
    at_col = lax.broadcasted_iota(jnp.int32, (128, 128), 1)
    same = (at_row // 4) % 2 == (at_col // 4) % 2
    eye = jnp.where(at_row == at_col, 1.0, 0.0)
    upper = (at_row // 4) % 2 == 0

    def grams(chunk):
        drain(in2.at[chunk, :, pl.ds(0, 7)], recv2.at[chunk])
        drain(in2.at[chunk, :, 0], local.at[CHUNKS + chunk])
        for half in range(2):
            blocks = []
            for k in range(2):
                both = in2[chunk, half, 4 * k : 4 * k + 4].reshape(16, 16, 128)
                a, b = both[:, :8], both[:, 8:]
                blocks.append(jnp.where(low, a, roll4(b)).reshape(128, 128))
                blocks.append(jnp.where(low, roll4(a), b).reshape(128, 128))
            whole = jnp.concatenate(blocks, axis=1)
            zbuf[chunk, half] = whole
            gram = lax.dot_general(
                whole, whole, (((1,), (1,)), ((), ())), precision=HIGHEST, preferred_element_type=jnp.float32
            )
            gram = jnp.where(same, gram, 0.0).reshape(8, 2, 8, 128)
            even, odd = gram[:, 0], gram[:, 1]
            even, odd = even + roll4(even), odd + roll4(odd)
            gsend[chunk, 64 * half : 64 * half + 64, :] = jnp.where(low8, even, odd).reshape(64, 128)
        gx[chunk, x] = gsend[chunk]
        for i in (2, 1, 3):
            remote(gsend.at[chunk], gx.at[chunk, x], xrecv.at[chunk], x_peer(i), 4)

    def iterate(chunk):
        drain(gx.at[chunk, pl.ds(0, 3)], xrecv.at[chunk])
        total = (gx[chunk, 0] + gx[chunk, 1]) + (gx[chunk, 2] + gx[chunk, 3])
        state = []
        for half in range(2):
            part = total[64 * half : 64 * half + 64].reshape(8, 8, 128)
            turned = roll4(part)
            gram = jnp.stack([jnp.where(low8, part, turned), jnp.where(low8, turned, part)], axis=1).reshape(128, 128)
            gram = jnp.where(same, gram, 0.0)
            diag = gram * eye
            one = jnp.sum(jnp.where(upper, diag, 0.0), keepdims=True) + 1e-06
            two = jnp.sum(jnp.where(upper, 0.0, diag), keepdims=True) + 1e-06
            scale = lax.rsqrt(jnp.where(upper, one, two))
            state.append([gram * scale * scale, None, scale])
        grams_now, scales = [one[0] for one in state], [one[2] for one in state]
        products = None
        for step in range(ITERS):
            parts = [split(v) for v in grams_now]
            squares = [dot6(p, p) for p in parts]
            mixed = [3.4445 * eye - 4.775 * g + 2.0315 * s for g, s in zip(grams_now, squares)]
            mixed_parts = [split(v) for v in mixed]
            if step < ITERS - 1:
                turned = [dot6(m, p) for m, p in zip(mixed_parts, parts)]
            if products is None:
                products = mixed
            else:
                products = [dot6(m, split(p)) for m, p in zip(mixed_parts, products)]
            if step < ITERS - 1:
                grams_now = [dot6(split(t), m) for t, m in zip(turned, mixed_parts)]
        return [split(product * scale) for product, scale in zip(products, scales)]

    def apply(chunk, products):
        for half in range(2):
            out = dot6(products[half], split(zbuf[chunk, half]))
            for k in range(2):
                c0 = out[:, 256 * k : 256 * k + 128].reshape(16, 8, 128)
                c1 = out[:, 256 * k + 128 : 256 * k + 256].reshape(16, 8, 128)
                a, b = jnp.where(low, c0, roll4(c1)), jnp.where(low, roll4(c0), c1)
                out2[chunk, half, 4 * k : 4 * k + 4] = jnp.concatenate([a, b], axis=1).reshape(4, 4, 16, 128)

    new_momentum(0)
    new_momentum(1)

    @pl.when(x != HUB)
    def _():
        pl.semaphore_wait(barrier, 13)

    @pl.when(x == HUB)
    def _():
        pl.semaphore_wait(barrier, 16)

    send1(0)
    send1(1)

    @pl.when(x == HUB)
    def _():
        for i in (2, 1, 3):
            pl.semaphore_signal(entered, inc=1, device_id=x_peer(i), device_id_type=MESH)

    new_momentum(2)
    new_momentum(3)
    pltpu.make_async_copy(weight, wbuf, wload).start()
    send2(0)
    send2(1)
    send1(2)
    send1(3)

    @pl.when(x != HUB)
    def _():
        pl.semaphore_wait(entered, 1)

    grams(0)
    grams(1)
    send2(2)

    def step(t):
        products = iterate(t)

        @pl.when(t == 0)
        def _():
            send2(3)

        apply(t, products)
        send3(t)

        @pl.when(t < 2)
        def _():
            grams(t + 2)

        @pl.when((t > 0) & (t < 3))
        def _():
            send4(t - 1)

    loop(0, CHUNKS, step)
    send4(2)
    send4(3)
    pltpu.make_async_copy(weight, wbuf, wload).wait()
    loop(0, CHUNKS, subtract)

    drain(out1.at[:, :, pl.ds(0, 3)], send.at[0])
    drain(out2.at[:, :, pl.ds(0, 7)], send.at[1])
    drain(out2.at[:, :, pl.ds(0, 7)], send.at[2])
    drain(out1.at[:, :, pl.ds(0, 3)], send.at[3])
    drain(gx.at[:, pl.ds(0, 3)], send.at[4])


def update(grad, moment, weight):
    f32 = jnp.float32
    whole = (32, CHUNKS, 32, 128)
    by_first = (CHUNKS, 2, 4, 8, 16, 128)
    by_second = (CHUNKS, 2, 8, 4, 16, 128)
    dma = pltpu.SemaphoreType.DMA
    return pl.pallas_call(
        kernel,
        out_shape=[jax.ShapeDtypeStruct(whole, f32)] * 2,
        in_specs=[pl.BlockSpec(memory_space=pltpu.HBM)] * 3,
        out_specs=[pl.BlockSpec(memory_space=pltpu.VMEM)] * 2,
        scratch_shapes=[
            pltpu.VMEM(whole, f32),
            pltpu.VMEM(whole, f32),
            pltpu.VMEM(whole, f32),
            pltpu.VMEM(by_first, f32),
            pltpu.VMEM(by_second, f32),
            pltpu.VMEM(by_second, f32),
            pltpu.VMEM((CHUNKS, 2, 128, 512), f32),
            pltpu.VMEM(by_second, f32),
            pltpu.VMEM(by_first, f32),
            pltpu.VMEM(by_first, f32),
            pltpu.VMEM((CHUNKS, 128, 128), f32),
            pltpu.VMEM((CHUNKS, 4, 128, 128), f32),
            dma((2 * CHUNKS,)),
            dma,
            dma((4 * CHUNKS,)),
            dma((5,)),
            dma((CHUNKS,)),
            dma((CHUNKS,)),
            dma((CHUNKS,)),
            dma((CHUNKS,)),
            dma((CHUNKS,)),
            pltpu.SemaphoreType.REGULAR,
        ],
        compiler_params=pltpu.CompilerParams(collective_id=0, has_side_effects=True, vmem_limit_bytes=40 * 1024 * 1024),
        name="update",
    )(grad, moment, weight)


def store(momentum, result, momentum_out, result_out, sems):
    copies = []
    for part in range(4):
        at = pl.ds(8 * part, 8)
        copies.append(pltpu.make_async_copy(momentum.at[at], momentum_out.at[at], sems.at[part]))
        copies.append(pltpu.make_async_copy(result.at[at], result_out.at[at], sems.at[4 + part]))
    for copy in copies:
        copy.start()
    for copy in copies:
        copy.wait()


def put_out(momentum, result):
    return pl.pallas_call(
        store,
        out_shape=[jax.ShapeDtypeStruct(momentum.shape, jnp.float32)] * 2,
        in_specs=[pl.BlockSpec(memory_space=pltpu.VMEM)] * 2,
        out_specs=[pl.BlockSpec(memory_space=pl.ANY)] * 2,
        scratch_shapes=[pltpu.SemaphoreType.DMA((8,))],
        compiler_params=pltpu.CompilerParams(vmem_limit_bytes=8 * 1024 * 1024),
        name="put_out",
    )(momentum, result)


def tiles(a):
    return a.reshape(512, 4, 2, 128).transpose(0, 2, 1, 3).reshape(32, CHUNKS, 32, 128)


def untiled(a):
    return a.reshape(512, 2, 4, 128).transpose(0, 2, 1, 3).reshape(512, 4, 256)


def on_device(grad_stack, moment_stack, weight_stack):
    momentum, result = update(*[pltpu.with_memory_space_constraint(tiles(a), pltpu.HBM) for a in (grad_stack, moment_stack, weight_stack)])
    momentum, result = put_out(momentum, result)
    return (untiled(result), untiled(momentum))


def solution(mesh):
    placed = (P(None, "rows", "cols"), P(None, "rows", "cols"), P(None, "rows", "cols"))
    return jax.shard_map(
        on_device,
        mesh=mesh,
        in_specs=placed,
        out_specs=(P(None, "rows", "cols"), P(None, "rows", "cols")),
        check_vma=False,
    )
```

```python
import jax
import jax.numpy as jnp
from jax import lax
from jax.experimental import pallas as pl
from jax.experimental.pallas import tpu as pltpu
from jax.sharding import PartitionSpec as P

MESH = pl.DeviceIdType.MESH
HIGHEST = lax.Precision.HIGHEST

hold_rate = 0.95
learn_rate = 1.0
ITERS = 5
CHUNKS = 4
HUB = 2


def split(a):
    high = a.astype(jnp.bfloat16)
    rest = a - high.astype(jnp.float32)
    middle = rest.astype(jnp.bfloat16)
    return high, middle, (rest - middle.astype(jnp.float32)).astype(jnp.bfloat16)


def dot6(a, b):
    (ah, am, al), (bh, bm, bl) = a, b
    n = bh.shape[1]
    wide, small = jnp.concatenate([ah, am], axis=1), jnp.concatenate([ah, al], axis=1)
    top, middle = jnp.concatenate([bh, bh], axis=0), jnp.concatenate([bm, bm], axis=0)
    rest = jnp.dot(small, jnp.concatenate([bl, bh], axis=0), preferred_element_type=jnp.float32)
    if n > 128:
        return (rest + jnp.dot(wide, middle, preferred_element_type=jnp.float32)) + jnp.dot(
            wide, top, preferred_element_type=jnp.float32
        )
    both = jnp.dot(wide, jnp.concatenate([top, middle], axis=1), preferred_element_type=jnp.float32)
    return (rest + both[:, n:]) + both[:, :n]


def kernel(
    grad, moment, weight, momentum, result,
    gbuf, mbuf, wbuf, out1, in1, in2, zbuf, out2, in3, in4, gsend, gx,
    load, wload, local, send, recv1, recv2, recv3, recv4, xrecv, entered,
):
    row, col = lax.axis_index("rows"), lax.axis_index("cols")
    z, y = row // 4, row % 4
    x, core = col // 2, col % 2
    first, second = (y, z), (z, y)

    def along_first(half, i):
        to = (first[half] + i) % 4
        to_row = z * 4 + to if half == 0 else to * 4 + y
        return to, {"rows": to_row, "cols": col}

    def along_second(half, i):
        to, to_core = (second[half] + i // 2) % 4, (core + i % 2) % 2
        to_row = to * 4 + y if half == 0 else z * 4 + to
        return to, to_core, {"rows": to_row, "cols": x * 2 + to_core}

    def x_peer(i):
        return {"rows": row, "cols": ((x + i) % 4) * 2 + core}

    def loop(start, stop, body):
        def one(i, carry):
            body(i)
            return carry

        lax.fori_loop(start, stop, one, 0)

    barrier = pltpu.get_barrier_semaphore()

    def greet(device):
        pl.semaphore_signal(barrier, inc=1, device_id=device, device_id_type=MESH)

    def fetch(chunk):
        pltpu.make_async_copy(grad.at[:, chunk], gbuf.at[:, chunk], load.at[chunk]).start()
        pltpu.make_async_copy(moment.at[:, chunk], mbuf.at[:, chunk], load.at[CHUNKS + chunk]).start()

    fetch(0)
    for i in (5, 4, 3, 2, 7, 6):
        for half in range(2):
            greet(along_second(half, i)[2])
    greet({"rows": row, "cols": x * 2 + (core + 1) % 2})

    @pl.when(x != HUB)
    def _():
        greet({"rows": row, "cols": HUB * 2 + core})

    for chunk in range(1, CHUNKS):
        fetch(chunk)

    def remote(src, dst, sem, device, which):
        pltpu.make_async_remote_copy(
            src_ref=src, dst_ref=dst, send_sem=send.at[which], recv_sem=sem, device_id=device, device_id_type=MESH
        ).start()

    def drain(ref, sem):
        pltpu.make_async_copy(ref, ref, sem).wait()

    def new_momentum(chunk):
        pltpu.make_async_copy(grad.at[:, chunk], gbuf.at[:, chunk], load.at[chunk]).wait()
        pltpu.make_async_copy(moment.at[:, chunk], mbuf.at[:, chunk], load.at[CHUNKS + chunk]).wait()
        for home in range(32):
            to_z, to_y, to_core = home // 8, (home // 2) % 4, home % 2
            value = hold_rate * mbuf[home, chunk] + gbuf[home, chunk]
            momentum[home, chunk] = value
            out1[chunk, 0, to_y, to_z * 2 + to_core] = value[:16]
            out1[chunk, 1, to_z, to_y * 2 + to_core] = value[16:]

    def send1(chunk):
        for half in range(2):
            own = first[half]
            pltpu.make_async_copy(out1.at[chunk, half, own], in1.at[chunk, half, :, own], local.at[chunk]).start()

        def one(i):
            for half in range(2):
                to, device = along_first(half, i)
                remote(out1.at[chunk, half, to], in1.at[chunk, half, :, first[half]], recv1.at[chunk], device, 0)

        for i in (2, 1, 3):
            one(i)

    def send2(chunk):
        drain(out1.at[chunk, :, pl.ds(0, 3)], recv1.at[chunk])
        drain(out1.at[chunk, :, 0], local.at[chunk])
        for half in range(2):
            pltpu.make_async_copy(
                in1.at[chunk, half, second[half] * 2 + core],
                in2.at[chunk, half, core * 4 + second[half]],
                local.at[CHUNKS + chunk],
            ).start()

        def one(i):
            for half in range(2):
                to, to_core, device = along_second(half, i)
                remote(
                    in1.at[chunk, half, to * 2 + to_core],
                    in2.at[chunk, half, core * 4 + second[half]],
                    recv2.at[chunk],
                    device,
                    1,
                )

        for i in (4, 5, 2, 3, 6, 7, 1):
            one(i)

    def send3(chunk):
        for half in range(2):
            pltpu.make_async_copy(
                out2.at[chunk, half, core * 4 + second[half]],
                in3.at[chunk, half, :, second[half] * 2 + core],
                local.at[2 * CHUNKS + chunk],
            ).start()

        def one(i):
            for half in range(2):
                to, to_core, device = along_second(half, i)
                remote(
                    out2.at[chunk, half, to_core * 4 + to],
                    in3.at[chunk, half, :, second[half] * 2 + core],
                    recv3.at[chunk],
                    device,
                    2,
                )

        for i in (4, 5, 2, 3, 6, 7, 1):
            one(i)

    def send4(chunk):
        drain(out2.at[chunk, :, pl.ds(0, 7)], recv3.at[chunk])
        drain(out2.at[chunk, :, 0], local.at[2 * CHUNKS + chunk])
        for half in range(2):
            own = first[half]
            pltpu.make_async_copy(in3.at[chunk, half, own], in4.at[chunk, half, own], local.at[3 * CHUNKS + chunk]).start()

        def one(i):
            for half in range(2):
                to, device = along_first(half, i)
                remote(in3.at[chunk, half, to], in4.at[chunk, half, first[half]], recv4.at[chunk], device, 3)

        for i in (2, 1, 3):
            one(i)

    def subtract(chunk):
        drain(in4.at[chunk, :, pl.ds(0, 3)], recv4.at[chunk])
        drain(in4.at[chunk, :, 0], local.at[3 * CHUNKS + chunk])
        for home in range(32):
            to_z, to_y, to_core = home // 8, (home // 2) % 4, home % 2
            result[home, chunk, :16] = wbuf[home, chunk, :16] - learn_rate * in4[chunk, 0, to_y, to_z * 2 + to_core]
            result[home, chunk, 16:] = wbuf[home, chunk, 16:] - learn_rate * in4[chunk, 1, to_z, to_y * 2 + to_core]

    def roll4(v):
        return pltpu.roll(v, 4, 1)

    low = lax.broadcasted_iota(jnp.int32, (16, 8, 128), 1) < 4
    low8 = lax.broadcasted_iota(jnp.int32, (8, 8, 128), 1) < 4
    at_row = lax.broadcasted_iota(jnp.int32, (128, 128), 0)
    at_col = lax.broadcasted_iota(jnp.int32, (128, 128), 1)
    same = (at_row // 4) % 2 == (at_col // 4) % 2
    eye = jnp.where(at_row == at_col, 1.0, 0.0)
    upper = (at_row // 4) % 2 == 0

    def grams(chunk):
        drain(in2.at[chunk, :, pl.ds(0, 7)], recv2.at[chunk])
        drain(in2.at[chunk, :, 0], local.at[CHUNKS + chunk])
        for half in range(2):
            blocks = []
            for k in range(2):
                both = in2[chunk, half, 4 * k : 4 * k + 4].reshape(16, 16, 128)
                a, b = both[:, :8], both[:, 8:]
                blocks.append(jnp.where(low, a, roll4(b)).reshape(128, 128))
                blocks.append(jnp.where(low, roll4(a), b).reshape(128, 128))
            whole = jnp.concatenate(blocks, axis=1)
            zbuf[chunk, half] = whole
            gram = lax.dot_general(
                whole, whole, (((1,), (1,)), ((), ())), precision=HIGHEST, preferred_element_type=jnp.float32
            )
            gram = jnp.where(same, gram, 0.0).reshape(8, 2, 8, 128)
            even, odd = gram[:, 0], gram[:, 1]
            even, odd = even + roll4(even), odd + roll4(odd)
            gsend[chunk, 64 * half : 64 * half + 64, :] = jnp.where(low8, even, odd).reshape(64, 128)
        gx[chunk, x] = gsend[chunk]
        for i in (2, 1, 3):
            remote(gsend.at[chunk], gx.at[chunk, x], xrecv.at[chunk], x_peer(i), 4)

    def iterate(chunk):
        drain(gx.at[chunk, pl.ds(0, 3)], xrecv.at[chunk])
        total = (gx[chunk, 0] + gx[chunk, 1]) + (gx[chunk, 2] + gx[chunk, 3])
        state = []
        for half in range(2):
            part = total[64 * half : 64 * half + 64].reshape(8, 8, 128)
            turned = roll4(part)
            gram = jnp.stack([jnp.where(low8, part, turned), jnp.where(low8, turned, part)], axis=1).reshape(128, 128)
            gram = jnp.where(same, gram, 0.0)
            diag = gram * eye
            one = jnp.sum(jnp.where(upper, diag, 0.0), keepdims=True) + 1e-06
            two = jnp.sum(jnp.where(upper, 0.0, diag), keepdims=True) + 1e-06
            scale = lax.rsqrt(jnp.where(upper, one, two))
            state.append([gram * scale * scale, None, scale])
        grams_now, scales = [one[0] for one in state], [one[2] for one in state]
        products = None
        for step in range(ITERS):
            parts = [split(v) for v in grams_now]
            squares = [dot6(p, p) for p in parts]
            mixed = [3.4445 * eye - 4.775 * g + 2.0315 * s for g, s in zip(grams_now, squares)]
            mixed_parts = [split(v) for v in mixed]
            if step < ITERS - 1:
                turned = [dot6(m, p) for m, p in zip(mixed_parts, parts)]
            if products is None:
                products = mixed
            else:
                products = [dot6(m, split(p)) for m, p in zip(mixed_parts, products)]
            if step < ITERS - 1:
                grams_now = [dot6(split(t), m) for t, m in zip(turned, mixed_parts)]
        return [split(product * scale) for product, scale in zip(products, scales)]

    def apply(chunk, products):
        for half in range(2):
            out = dot6(products[half], split(zbuf[chunk, half]))
            for k in range(2):
                c0 = out[:, 256 * k : 256 * k + 128].reshape(16, 8, 128)
                c1 = out[:, 256 * k + 128 : 256 * k + 256].reshape(16, 8, 128)
                a, b = jnp.where(low, c0, roll4(c1)), jnp.where(low, roll4(c0), c1)
                out2[chunk, half, 4 * k : 4 * k + 4] = jnp.concatenate([a, b], axis=1).reshape(4, 4, 16, 128)

    new_momentum(0)

    @pl.when(x != HUB)
    def _():
        pl.semaphore_wait(barrier, 13)

    @pl.when(x == HUB)
    def _():
        pl.semaphore_wait(barrier, 16)
        for i in (2, 1, 3):
            pl.semaphore_signal(entered, inc=1, device_id=x_peer(i), device_id_type=MESH)

    send1(0)
    new_momentum(1)
    send1(1)
    new_momentum(2)
    new_momentum(3)
    pltpu.make_async_copy(weight, wbuf, wload).start()
    send2(0)
    send2(1)
    send1(2)

    @pl.when(x != HUB)
    def _():
        pl.semaphore_wait(entered, 1)

    grams(0)
    send1(3)
    grams(1)
    send2(2)

    def step(t):
        products = iterate(t)

        @pl.when(t == 0)
        def _():
            send2(3)

        apply(t, products)
        send3(t)

        @pl.when(t < 2)
        def _():
            grams(t + 2)

        @pl.when((t > 0) & (t < 3))
        def _():
            send4(t - 1)

    loop(0, CHUNKS, step)
    send4(2)
    send4(3)
    pltpu.make_async_copy(weight, wbuf, wload).wait()
    loop(0, CHUNKS, subtract)

    drain(out1.at[:, :, pl.ds(0, 3)], send.at[0])
    drain(out2.at[:, :, pl.ds(0, 7)], send.at[1])
    drain(out2.at[:, :, pl.ds(0, 7)], send.at[2])
    drain(out1.at[:, :, pl.ds(0, 3)], send.at[3])
    drain(gx.at[:, pl.ds(0, 3)], send.at[4])


def update(grad, moment, weight):
    f32 = jnp.float32
    whole = (32, CHUNKS, 32, 128)
    by_first = (CHUNKS, 2, 4, 8, 16, 128)
    by_second = (CHUNKS, 2, 8, 4, 16, 128)
    dma = pltpu.SemaphoreType.DMA
    return pl.pallas_call(
        kernel,
        out_shape=[jax.ShapeDtypeStruct(whole, f32)] * 2,
        in_specs=[pl.BlockSpec(memory_space=pltpu.HBM)] * 3,
        out_specs=[pl.BlockSpec(memory_space=pltpu.VMEM)] * 2,
        scratch_shapes=[
            pltpu.VMEM(whole, f32),
            pltpu.VMEM(whole, f32),
            pltpu.VMEM(whole, f32),
            pltpu.VMEM(by_first, f32),
            pltpu.VMEM(by_second, f32),
            pltpu.VMEM(by_second, f32),
            pltpu.VMEM((CHUNKS, 2, 128, 512), f32),
            pltpu.VMEM(by_second, f32),
            pltpu.VMEM(by_first, f32),
            pltpu.VMEM(by_first, f32),
            pltpu.VMEM((CHUNKS, 128, 128), f32),
            pltpu.VMEM((CHUNKS, 4, 128, 128), f32),
            dma((2 * CHUNKS,)),
            dma,
            dma((4 * CHUNKS,)),
            dma((5,)),
            dma((CHUNKS,)),
            dma((CHUNKS,)),
            dma((CHUNKS,)),
            dma((CHUNKS,)),
            dma((CHUNKS,)),
            pltpu.SemaphoreType.REGULAR,
        ],
        compiler_params=pltpu.CompilerParams(collective_id=0, has_side_effects=True, vmem_limit_bytes=40 * 1024 * 1024),
        name="update",
    )(grad, moment, weight)


def store(momentum, result, momentum_out, result_out, sems):
    copies = []
    for part in range(4):
        at = pl.ds(8 * part, 8)
        copies.append(pltpu.make_async_copy(momentum.at[at], momentum_out.at[at], sems.at[part]))
        copies.append(pltpu.make_async_copy(result.at[at], result_out.at[at], sems.at[4 + part]))
    for copy in copies:
        copy.start()
    for copy in copies:
        copy.wait()


def put_out(momentum, result):
    return pl.pallas_call(
        store,
        out_shape=[jax.ShapeDtypeStruct(momentum.shape, jnp.float32)] * 2,
        in_specs=[pl.BlockSpec(memory_space=pltpu.VMEM)] * 2,
        out_specs=[pl.BlockSpec(memory_space=pl.ANY)] * 2,
        scratch_shapes=[pltpu.SemaphoreType.DMA((8,))],
        compiler_params=pltpu.CompilerParams(vmem_limit_bytes=8 * 1024 * 1024),
        name="put_out",
    )(momentum, result)


def tiles(a):
    return a.reshape(512, 4, 2, 128).transpose(0, 2, 1, 3).reshape(32, CHUNKS, 32, 128)


def untiled(a):
    return a.reshape(512, 2, 4, 128).transpose(0, 2, 1, 3).reshape(512, 4, 256)


def on_device(grad_stack, moment_stack, weight_stack):
    momentum, result = update(*[pltpu.with_memory_space_constraint(tiles(a), pltpu.HBM) for a in (grad_stack, moment_stack, weight_stack)])
    momentum, result = put_out(momentum, result)
    return (untiled(result), untiled(momentum))


def solution(mesh):
    placed = (P(None, "rows", "cols"), P(None, "rows", "cols"), P(None, "rows", "cols"))
    return jax.shard_map(
        on_device,
        mesh=mesh,
        in_specs=placed,
        out_specs=(P(None, "rows", "cols"), P(None, "rows", "cols")),
        check_vma=False,
    )
```
